16 devices in a mesh: dp: 2 (over y, z), vp: 8 (over x, core).
Axes of the slice: x: 4, y: 2, z: 1, core: 2. Of those that a mesh axis runs over, the one named last changes fastest.
The devices are a block of a 4x4x8 slice.
Arguments:
- hidden: bfloat16 [1024, 6144], P('dp'), parts along dimension 0
- w_head: bfloat16 [6144, 32768], P(None, 'vp')
- inv_temp: float32 [1024], P('dp'), parts along dimension 0
- target_ids: int32 [1024], P('dp'), parts along dimension 0
Outputs:
- output 1: float32 [1024, 32768], P(('dp', 'vp')), parts along dimension 0
- output 2: float32 [1024], P('dp'), parts along dimension 0
There are 2 independent parts. The reference program is written for one: setup_inputs(seed, part) draws one part's arguments, and reference() takes and returns one part's arrays. A program takes and returns all parts, laid end to end along the dimension named above; an argument that names none is the same for every part.
All inputs are finite; a program needn't handle non-finite values.
Results may differ from the reference program's by a relative error of at most 0.001.
Values are sent between devices in bfloat16 or wider.
A program may use at most 768 MiB of HBM per device.

```python
import math
import jax
import jax.numpy as jnp
from jax import lax

BATCH = 512
HIDDEN = 6144
VOCAB = 32768
W_ROW_BLOCK = 256


def draw_head(key, direction, profile):
    num_blocks = HIDDEN // W_ROW_BLOCK
    dir_blocks = direction.reshape(num_blocks, W_ROW_BLOCK)

    def one_block(block_args):
        block_idx, dir_rows = block_args
        noise_rows = jax.random.normal(jax.random.fold_in(key, block_idx), (W_ROW_BLOCK, VOCAB), jnp.float32)
        head_rows = (noise_rows + dir_rows[:, None] * profile[None, :]) * (HIDDEN ** -0.5)
        return head_rows.astype(jnp.bfloat16)

    blocks = lax.map(one_block, (jnp.arange(num_blocks), dir_blocks))
    return blocks.reshape(HIDDEN, VOCAB)


def setup_inputs(seed: int = 0, part: int = 0) -> dict:
    base_key = jax.random.key(seed)
    shared_key = jax.random.fold_in(base_key, 1)
    part_key = jax.random.fold_in(jax.random.fold_in(base_key, 2), part)
    key_dir, key_head = jax.random.split(shared_key)
    key_hid, key_gain, key_temp, key_ids = jax.random.split(part_key, 4)
    direction = jax.random.normal(key_dir, (HIDDEN,), jnp.float32)
    vocab_pos = jnp.arange(VOCAB, dtype=jnp.float32) / VOCAB
    profile = 1.5 * jnp.exp(-8.0 * vocab_pos)
    w_head = draw_head(key_head, direction, profile)
    row_gain = 2.0 + 0.5 * jax.random.normal(key_gain, (BATCH, 1), jnp.float32)
    hidden = jax.random.normal(key_hid, (BATCH, HIDDEN), jnp.float32) + row_gain * direction[None, :] * (HIDDEN ** -0.5)
    row_pos = jnp.arange(BATCH)
    log_temp = jax.random.uniform(key_temp, (BATCH,), jnp.float32, minval=math.log(0.5), maxval=math.log(32.0))
    inv_temp = jnp.where(row_pos == 0, 32.0, jnp.exp(log_temp))
    target_ids = jax.random.randint(key_ids, (BATCH,), 0, VOCAB, dtype=jnp.int32)
    target_ids = jnp.where(row_pos == 1, VOCAB - 1, target_ids)
    return {"hidden": hidden.astype(jnp.bfloat16), "w_head": w_head, "inv_temp": inv_temp, "target_ids": target_ids}


def reference(hidden, w_head, inv_temp, target_ids):
    logits = jnp.dot(hidden, w_head, preferred_element_type=jnp.float32)
    scaled = logits * inv_temp[:, None]
    row_max = jnp.max(scaled, axis=1, keepdims=True)
    exp_vals = jnp.exp(scaled - row_max)
    probabilities = exp_vals / jnp.sum(exp_vals, axis=1, keepdims=True)
    cdf_table = jnp.cumsum(probabilities, axis=1)
    cdf_at_target = jnp.take_along_axis(cdf_table, target_ids[:, None], axis=1)[:, 0]
    return cdf_table, cdf_at_target
```

```python
import functools

import jax
import jax.numpy as jnp
from jax import lax
from jax.experimental import pallas as pl
from jax.experimental.pallas import tpu as pltpu
from jax.sharding import PartitionSpec as P

MESH = pl.DeviceIdType.MESH
F32 = jnp.float32
BF16 = jnp.bfloat16
TILE = 256
LANES = 128
GROUP = 4
PEERS = ((2, 0), (2, 1), (0, 1), (1, 0), (3, 0), (1, 1), (3, 1))
EARLY = 3


def kernel(chips, h_hbm, w_hbm, temp_hbm, ids_hbm, table, picked,
           h, w, z, land, temp_row, ids_row, temp, ids, peak, stat_out, stats, rows, cols, inv_s, top, carry, tri,
           h_sem, w_sem, row_sem, send_sem, recv_sem, stat_send, stat_recv):
    n = 2 * chips
    me = lax.axis_index("vp")
    x, c = me // 2, me % 2
    batch, depth = h_hbm.shape
    vocab = w_hbm.shape[1]
    tiles = vocab // TILE
    own = batch // n
    pair = 2 * own

    def peer(i):
        dx, dc = PEERS[i]
        return lax.rem(x + dx, chips) * 2 + lax.rem(c + dc, 2)

    def source(i):
        dx, dc = PEERS[i]
        return lax.rem(x + chips - dx, chips) * 2 + lax.rem(c + dc, 2)

    def chip_rows(j):
        return pl.multiple_of(lax.rem(x + 2 + j, chips) * pair, pair)

    def h_copy(j):
        r = chip_rows(j)
        return pltpu.make_async_copy(h_hbm.at[pl.ds(r, pair), :], h.at[pl.ds(r, pair), :], h_sem.at[j])

    def w_copy(t):
        col = pl.multiple_of(t * TILE, TILE)
        slot = lax.rem(t, 2)
        return pltpu.make_async_copy(w_hbm.at[:, pl.ds(col, TILE)], w.at[slot], w_sem.at[slot])

    def send(i, t):
        to = peer(i)
        r = pl.multiple_of(to * own, own)
        return pltpu.make_async_remote_copy(
            src_ref=z.at[t, pl.ds(r, own), :], dst_ref=land.at[i, t], send_sem=send_sem, recv_sem=recv_sem.at[i, t],
            device_id={"vp": to}, device_id_type=MESH)

    def send_stat(i):
        return pltpu.make_async_remote_copy(
            src_ref=stat_out, dst_ref=stats.at[me], send_sem=stat_send.at[i], recv_sem=stat_recv.at[i],
            device_id={"vp": peer(i)}, device_id_type=MESH)

    def recv_stat(i):
        return pltpu.make_async_remote_copy(
            src_ref=stat_out, dst_ref=stats.at[source(i)], send_sem=stat_send.at[i], recv_sem=stat_recv.at[i],
            device_id={"vp": peer(i)}, device_id_type=MESH)

    temp_copy = pltpu.make_async_copy(temp_hbm, temp_row, row_sem.at[0])
    ids_copy = pltpu.make_async_copy(ids_hbm, ids_row, row_sem.at[1])
    temp_copy.start()
    h_copy(0).start()
    w_copy(0).start()
    for j in range(1, chips):
        h_copy(j).start()
    ids_copy.start()

    barrier = pltpu.get_barrier_semaphore()
    for i in range(n - 1):
        pl.semaphore_signal(barrier, inc=1, device_id={"vp": peer(i)}, device_id_type=MESH)

    row_id = lax.broadcasted_iota(jnp.int32, (TILE, TILE), 0)
    col_id = lax.broadcasted_iota(jnp.int32, (TILE, TILE), 1)
    tri[...] = jnp.where(row_id <= col_id, 1.0, 0.0).astype(BF16)
    temp_copy.wait()
    temp[...] = jnp.broadcast_to(temp_row[...], (LANES, batch)).T

    def tile_rows(t, slot, r, size, first):
        acc = jnp.dot(h[pl.ds(r, size), :], w[slot], preferred_element_type=F32)
        by = temp[pl.ds(r, size), :]
        left, right = acc[:, :LANES] * by, acc[:, LANES:] * by
        z[t, pl.ds(r, size), :LANES] = left
        z[t, pl.ds(r, size), LANES:] = right
        best = jnp.maximum(left, right)
        if not first:
            best = jnp.maximum(best, peak[pl.ds(r, size), :])
        peak[pl.ds(r, size), :] = best

    h_copy(0).wait()
    w_copy(0).wait()
    w_copy(1).start()
    tile_rows(0, 0, chip_rows(0), pair, True)
    pl.semaphore_wait(barrier, n - 1)
    send(0, 0).start()
    send(1, 0).start()

    @pl.loop(1, chips)
    def _(j):
        h_copy(j).wait()
        tile_rows(0, 0, chip_rows(j), pair, True)

    send(2, 0).start()

    @pl.loop(1, tiles)
    def _(t):
        @pl.when(t + 1 < tiles)
        def _():
            w_copy(t + 1).start()
        w_copy(t).wait()
        tile_rows(t, lax.rem(t, 2), 0, batch, False)
        for i in range(EARLY):
            send(i, t).start()

    ids_copy.wait()
    ids[...] = jnp.broadcast_to(ids_row[...], (LANES, batch)).T
    lane = lax.broadcasted_iota(jnp.int32, (own, LANES), 1)

    @pl.loop(0, n)
    def _(b):
        rs = pl.ds(pl.multiple_of(b * own, own), own)
        most = jnp.broadcast_to(jnp.max(peak[rs, :], axis=1, keepdims=True), (own, LANES))
        target = ids[rs, :] - (me * vocab) - lane

        def add(t, sums):
            total, below = sums
            for half in range(2):
                e = jnp.exp(z[t, rs, half * LANES:(half + 1) * LANES] - most)
                total = total + e
                below = below + jnp.where(target >= t * TILE + half * LANES, e, 0.0)
            return total, below

        zero = jnp.zeros((own, LANES), F32)
        total, below = lax.fori_loop(0, tiles, add, (zero, zero))
        total = jnp.sum(total, axis=1, keepdims=True)
        below = jnp.sum(below, axis=1, keepdims=True)
        peak[rs, :] = jnp.where(lane == 0, most, jnp.where(lane == 1, total, below))

    flipped = peak[...].T
    stat_out[...] = flipped[:4, :]
    stats[me] = flipped[:4, :]
    for i in range(n - 1):
        send_stat(i).start()

    @pl.loop(0, tiles)
    def _(t):
        for i in range(EARLY, n - 1):
            send(i, t).start()

    for i in range(n - 1):
        recv_stat(i).wait_recv()

    most = stats[0, 0:1, :]
    for d in range(1, n):
        most = jnp.maximum(most, stats[d, 0:1, :])
    mass = jnp.zeros_like(most)
    below = jnp.zeros_like(most)
    for d in range(n):
        rows[8 + d:9 + d, :] = mass
        scale = jnp.exp(stats[d, 0:1, :] - most)
        mass = mass + stats[d, 1:2, :] * scale
        below = below + stats[d, 2:3, :] * scale
    rows[0:1, :] = most
    rows[1:2, :] = mass
    picked[...] = below / mass

    mine = rows[:, pl.ds(pl.multiple_of(x * pair, pair), pair)]
    cols[...] = jnp.concatenate([mine, jnp.zeros((LANES - 16, LANES), F32)], axis=0).T
    mine = cols[pl.ds(pl.multiple_of(c * own, own), own), :]
    top[...] = jnp.broadcast_to(mine[:, 0:1], (own, TILE))
    scale = 1.0 / jnp.broadcast_to(mine[:, 1:2], (own, TILE))
    inv_s[...] = scale
    for i in range(n):
        d = source(i) if i < n - 1 else me
        start = jnp.sum(jnp.where(lane == 8 + d, mine, 0.0), axis=1, keepdims=True)
        carry[i] = jnp.broadcast_to(start, (own, TILE)) * scale

    def finish(i, d, t, count, read):
        e = jnp.concatenate([jnp.exp(read(t + k) - top[...]) * inv_s[...] for k in range(count)], axis=0)
        hi = e.astype(BF16)
        rest = e - hi.astype(F32)
        mid = rest.astype(BF16)
        low = (rest - mid.astype(F32)).astype(BF16)
        run = jnp.dot(hi, tri[...], preferred_element_type=F32)
        run = run + jnp.dot(mid, tri[...], preferred_element_type=F32)
        run = run + jnp.dot(low, tri[...], preferred_element_type=F32)
        base = carry[i]
        for k in range(count):
            part = run[k * own:(k + 1) * own, :]
            col = pl.multiple_of(d * vocab + (t + k) * TILE, TILE)
            table[:, pl.ds(col, TILE)] = part + base
            base = base + jnp.broadcast_to(part[:, TILE - 1:], (own, TILE))
        carry[i] = base

    my_rows = pl.ds(pl.multiple_of(me * own, own), own)

    @pl.loop(0, tiles // GROUP)
    def _(g):
        finish(n - 1, me, g * GROUP, GROUP, lambda t: z[t, my_rows, :])

    def arrive(i, t, count):
        for k in range(count):
            pltpu.make_async_copy(land.at[i, t + k], land.at[i, t + k], recv_sem.at[i, t + k]).wait()

    def source_of(i):
        dx = jnp.int32(0)
        dc = jnp.int32(0)
        for k, (kx, kc) in enumerate(PEERS):
            dx = dx + jnp.where(i == k, kx, 0)
            dc = dc + jnp.where(i == k, kc, 0)
        return lax.rem(x + chips - dx, chips) * 2 + lax.rem(c + dc, 2)

    def step(i, t, count):
        arrive(i, t, count)
        finish(i, source_of(i), t, count, lambda u: land[i, u])

    groups = tiles // GROUP

    @pl.loop(0, EARLY * groups)
    def _(k):
        step(k // groups, lax.rem(k, groups) * GROUP, GROUP)

    late = n - 1 - EARLY

    @pl.loop(0, late * (groups - 1))
    def _(k):
        step(EARLY + lax.rem(k, late), (k // late) * GROUP, GROUP)

    @pl.loop(0, late * GROUP)
    def _(k):
        step(EARLY + lax.rem(k, late), tiles - GROUP + k // late, 1)

    pltpu.make_async_copy(land, land, send_sem).wait()
    for i in range(n - 1):
        send_stat(i).wait_send()


def solution(mesh):
    n = mesh.shape["vp"]
    chips = n // 2

    def local_step(hidden, w_local, inv_temp, target_ids):
        batch, depth = hidden.shape
        vocab = w_local.shape[1]
        tiles = vocab // TILE
        own = batch // n
        hbm = pl.BlockSpec(memory_space=pltpu.HBM)
        vmem = pl.BlockSpec(memory_space=pltpu.VMEM)
        dma = pltpu.SemaphoreType.DMA
        table, picked = pl.pallas_call(
            functools.partial(kernel, chips),
            out_shape=(pltpu.VMEM((own, n * vocab), F32), jax.ShapeDtypeStruct((1, batch), F32)),
            in_specs=[hbm] * 4,
            out_specs=(vmem, vmem),
            scratch_shapes=[
                pltpu.VMEM((batch, depth), BF16),
                pltpu.VMEM((2, depth, TILE), BF16),
                pltpu.VMEM((tiles, batch, TILE), F32),
                pltpu.VMEM((n - 1, tiles, own, TILE), F32),
                pltpu.VMEM((1, batch), F32),
                pltpu.VMEM((1, batch), jnp.int32),
                pltpu.VMEM((batch, LANES), F32),
                pltpu.VMEM((batch, LANES), jnp.int32),
                pltpu.VMEM((batch, LANES), F32),
                pltpu.VMEM((4, batch), F32),
                pltpu.VMEM((n, 4, batch), F32),
                pltpu.VMEM((16, batch), F32),
                pltpu.VMEM((LANES, LANES), F32),
                pltpu.VMEM((own, TILE), F32),
                pltpu.VMEM((own, TILE), F32),
                pltpu.VMEM((n, own, TILE), F32),
                pltpu.VMEM((TILE, TILE), BF16),
                dma((chips,)), dma((2,)), dma((2,)), dma, dma((n - 1, tiles)), dma((n - 1,)), dma((n - 1,)),
            ],
            compiler_params=pltpu.CompilerParams(
                collective_id=0, has_side_effects=True, vmem_limit_bytes=52 * 2**20),
        )(hidden, w_local, inv_temp.reshape(1, batch), target_ids.reshape(1, batch))
        return table, picked.reshape(batch)

    return jax.shard_map(
        local_step,
        mesh=mesh,
        in_specs=(P("dp", None), P(None, "vp"), P("dp"), P("dp")),
        out_specs=(P(("dp", "vp"), None), P("dp")),
        check_vma=False,
    )
```

```python
import functools

import jax
import jax.numpy as jnp
from jax import lax
from jax.experimental import pallas as pl
from jax.experimental.pallas import tpu as pltpu
from jax.sharding import PartitionSpec as P

MESH = pl.DeviceIdType.MESH
F32 = jnp.float32
BF16 = jnp.bfloat16
TILE = 256
LANES = 128
GROUP = 4
PIECES = 4
PEERS = ((2, 0), (2, 1), (0, 1), (1, 0), (3, 0), (1, 1), (3, 1))
EARLY = 3
CHIP_ORDER = (2, 1, 3, 0)


def kernel(chips, h_hbm, w_hbm, temp_hbm, ids_hbm, table, picked,
           h, w, z, land, temp_row, ids_row, temp, ids, peak, stat_out, stats, pick, cols, inv_s, top, carry, tri,
           h_sem, w_sem, first_sem, row_sem, send_sem, recv_sem, stat_send, stat_recv, pick_send, pick_recv):
    n = 2 * chips
    me = lax.axis_index("vp")
    x, c = me // 2, me % 2
    batch, depth = h_hbm.shape
    vocab = w_hbm.shape[1]
    tiles = vocab // TILE
    own = batch // n
    pair = 2 * own
    piece = depth // PIECES

    def peer(i):
        dx, dc = PEERS[i]
        return lax.rem(x + dx, chips) * 2 + lax.rem(c + dc, 2)

    def source(i):
        dx, dc = PEERS[i]
        return lax.rem(x + chips - dx, chips) * 2 + lax.rem(c + dc, 2)

    def held(dx):
        return CHIP_ORDER.index(dx) * pair

    def peer_rows(i):
        dx, dc = PEERS[i]
        return pl.ds(pl.multiple_of(held(dx) + lax.rem(c + dc, 2) * own, own), own)

    def whole_rows(j):
        return pl.ds(pl.multiple_of(lax.rem(x + CHIP_ORDER[j], chips) * pair, pair), pair)

    def h_copy(j):
        return pltpu.make_async_copy(h_hbm.at[whole_rows(j), :], h.at[j * pair:(j + 1) * pair, :], h_sem.at[j])

    def turned(row):
        parts = [row[:, whole_rows(j)] for j in range(chips)]
        return jnp.broadcast_to(jnp.concatenate(parts, axis=1), (LANES, batch)).T

    def w_copy(t):
        col = pl.multiple_of(lax.rem(t, tiles) * TILE, TILE)
        slot = lax.rem(t, 2)
        return pltpu.make_async_copy(w_hbm.at[:, pl.ds(col, TILE)], w.at[slot], w_sem.at[slot])

    def first_copies(k):
        ks = slice(k * piece, (k + 1) * piece)
        return (pltpu.make_async_copy(w_hbm.at[ks, :LANES], w.at[0, ks, :LANES], first_sem.at[0, k]),
                pltpu.make_async_copy(h_hbm.at[whole_rows(0), ks], h.at[:pair, ks], first_sem.at[1, k]))

    second_copy = pltpu.make_async_copy(w_hbm.at[:, LANES:TILE], w.at[0, :, LANES:], w_sem.at[0])

    def remote(src, dst, send, recv, to):
        return pltpu.make_async_remote_copy(
            src_ref=src, dst_ref=dst, send_sem=send, recv_sem=recv, device_id={"vp": to}, device_id_type=MESH)

    def send(i, t):
        return remote(z.at[t, peer_rows(i), :], land.at[i, t], send_sem, recv_sem.at[i, t], peer(i))

    def send_half(i, half):
        ls = slice(half * LANES, (half + 1) * LANES)
        return remote(z.at[0, peer_rows(i), ls], land.at[i, 0, :, ls], send_sem, recv_sem.at[i, 0], peer(i))

    def send_stat(i):
        at = stat_out.at[CHIP_ORDER.index(PEERS[i][0])]
        return remote(at, stats.at[me], stat_send.at[i], stat_recv.at[i], peer(i))

    def recv_stat(i):
        return remote(stat_out.at[0], stats.at[source(i)], stat_send.at[i], stat_recv.at[i], peer(i))

    def send_pick(dx):
        to = lax.rem(x + dx, chips) * 2 + c
        return remote(pick.at[x], pick.at[x], pick_send.at[dx], pick_recv.at[dx], to)

    def recv_pick(dx):
        at = pick.at[lax.rem(x + chips - dx, chips)]
        return remote(at, at, pick_send.at[dx], pick_recv.at[dx], lax.rem(x + dx, chips) * 2 + c)

    barrier = pltpu.get_barrier_semaphore()
    for i in range(n - 1):
        pl.semaphore_signal(barrier, inc=1, device_id={"vp": peer(i)}, device_id_type=MESH)
    temp_copy = pltpu.make_async_copy(temp_hbm, temp_row, row_sem.at[0])
    ids_copy = pltpu.make_async_copy(ids_hbm, ids_row, row_sem.at[1])
    temp_copy.start()
    for k in range(PIECES):
        for copy in first_copies(k):
            copy.start()
    second_copy.start()
    for j in (1, 2):
        h_copy(j).start()
    temp_copy.wait()
    temp[...] = turned(temp_row)

    acc = jnp.zeros((pair, LANES), F32)
    for k in range(PIECES):
        for copy in first_copies(k):
            copy.wait()
        ks = slice(k * piece, (k + 1) * piece)
        acc = acc + jnp.dot(h[:pair, ks], w[0, ks, :LANES], preferred_element_type=F32)
    acc = acc * temp[:pair, :]
    z[0, :pair, :LANES] = acc
    peak[:pair, :] = acc
    pl.semaphore_wait(barrier, n - 1)
    for i in range(2):
        send_half(i, 0).start()
    w_copy(1).start()
    h_copy(3).start()
    ids_copy.start()
    second_copy.wait()
    acc = jnp.dot(h[:pair, :], w[0, :, LANES:], preferred_element_type=F32) * temp[:pair, :]
    z[0, :pair, LANES:] = acc
    peak[:pair, :] = jnp.maximum(peak[:pair, :], acc)
    for i in range(2):
        send_half(i, 1).start()

    def tile_rows(t, slot, rs):
        acc = jnp.dot(h[rs, :], w[slot], preferred_element_type=F32)
        by = temp[rs, :]
        left, right = acc[:, :LANES] * by, acc[:, LANES:] * by
        z[t, rs, :LANES] = left
        z[t, rs, LANES:] = right
        return jnp.maximum(left, right)

    h_copy(1).wait()
    h_copy(2).wait()
    near = pl.ds(pair, 2 * pair)
    peak[near, :] = tile_rows(0, 0, near)
    for i in range(EARLY, n - 1):
        send(i, 0).start()
    here = pl.ds(3 * pair, pair)
    peak[here, :] = jnp.full((pair, LANES), -jnp.inf, F32)
    h_copy(3).wait()

    @pl.loop(1, tiles)
    def _(t):
        w_copy(t + 1).start()
        w_copy(t).wait()
        best = tile_rows(t, lax.rem(t, 2), pl.ds(0, batch))
        for i in range(EARLY):
            send(i, t).start()
        peak[...] = jnp.maximum(peak[...], best)

    w_copy(tiles).wait()
    peak[here, :] = jnp.maximum(peak[here, :], tile_rows(0, 0, here))
    send(2, 0).start()

    ids_copy.wait()
    ids[...] = turned(ids_row)
    lane = lax.broadcasted_iota(jnp.int32, (own, LANES), 1)

    @pl.loop(0, n)
    def _(b):
        rs = pl.ds(pl.multiple_of(b * own, own), own)
        most = jnp.broadcast_to(jnp.max(peak[rs, :], axis=1, keepdims=True), (own, LANES))
        target = ids[rs, :] - (me * vocab) - lane

        def add(t, sums):
            total, below = sums
            for half in range(2):
                e = jnp.exp(z[t, rs, half * LANES:(half + 1) * LANES] - most)
                total = total + e
                below = below + jnp.where(target >= t * TILE + half * LANES, e, 0.0)
            return total, below

        zero = jnp.zeros((own, LANES), F32)
        total, below = lax.fori_loop(0, tiles, add, (zero, zero))
        total = jnp.sum(total, axis=1, keepdims=True)
        below = jnp.sum(below, axis=1, keepdims=True)
        peak[rs, :] = jnp.where(lane == 0, most, jnp.where(lane == 1, total, below))

    flipped = peak[...].T
    for j in range(chips):
        stat_out[j] = flipped[:4, j * pair:(j + 1) * pair]
    stats[me] = stat_out[CHIP_ORDER.index(0)]
    for i in range(n - 1):
        send_stat(i).start()

    def send_near(first, last):
        @pl.loop(first, last)
        def _(t):
            for i in range(EARLY, n - 1):
                send(i, t).start()

    send_near(1, tiles // 2)
    row_id = lax.broadcasted_iota(jnp.int32, (TILE, TILE), 0)
    col_id = lax.broadcasted_iota(jnp.int32, (TILE, TILE), 1)
    tri[...] = jnp.where(row_id <= col_id, 1.0, 0.0).astype(BF16)
    for i in range(n - 1):
        recv_stat(i).wait_recv()

    most = stats[0, 0:1, :]
    for d in range(1, n):
        most = jnp.maximum(most, stats[d, 0:1, :])
    mass = jnp.zeros_like(most)
    below = jnp.zeros_like(most)
    lower = []
    for d in range(n):
        lower.append(mass)
        scale = jnp.exp(stats[d, 0:1, :] - most)
        mass = mass + stats[d, 1:2, :] * scale
        below = below + stats[d, 2:3, :] * scale
    pick[x] = below / mass
    for dx in range(1, chips):
        send_pick(dx).start()
    send_near(tiles // 2, tiles)

    mine = jnp.concatenate(lower + [most, mass, jnp.zeros((LANES - n - 2, pair), F32)], axis=0)
    cols[...] = mine.T
    mine = cols[pl.ds(pl.multiple_of(c * own, own), own), :]
    top[...] = jnp.broadcast_to(mine[:, n:n + 1], (own, TILE))
    scale = 1.0 / jnp.broadcast_to(mine[:, n + 1:n + 2], (own, TILE))
    inv_s[...] = scale
    for i in range(n):
        d = source(i) if i < n - 1 else me
        start = jnp.sum(jnp.where(lane == d, mine, 0.0), axis=1, keepdims=True)
        carry[i] = jnp.broadcast_to(start, (own, TILE)) * scale

    def finish(i, d, t, count, read):
        e = jnp.concatenate([jnp.exp(read(t + k) - top[...]) * inv_s[...] for k in range(count)], axis=0)
        hi = e.astype(BF16)
        rest = e - hi.astype(F32)
        mid = rest.astype(BF16)
        low = (rest - mid.astype(F32)).astype(BF16)
        run = jnp.dot(hi, tri[...], preferred_element_type=F32)
        run = run + jnp.dot(mid, tri[...], preferred_element_type=F32)
        run = run + jnp.dot(low, tri[...], preferred_element_type=F32)
        base = carry[i]
        for k in range(count):
            part = run[k * own:(k + 1) * own, :]
            col = pl.multiple_of(d * vocab + (t + k) * TILE, TILE)
            table[:, pl.ds(col, TILE)] = part + base
            base = base + jnp.broadcast_to(part[:, TILE - 1:], (own, TILE))
        carry[i] = base

    my_rows = pl.ds(pl.multiple_of(held(0) + c * own, own), own)

    @pl.loop(0, tiles // GROUP)
    def _(g):
        finish(n - 1, me, g * GROUP, GROUP, lambda t: z[t, my_rows, :])

    def source_of(i):
        dx = jnp.int32(0)
        dc = jnp.int32(0)
        for k, (kx, kc) in enumerate(PEERS):
            dx = dx + jnp.where(i == k, kx, 0)
            dc = dc + jnp.where(i == k, kc, 0)
        return lax.rem(x + chips - dx, chips) * 2 + lax.rem(c + dc, 2)

    def step(i, t, count):
        for k in range(count):
            pltpu.make_async_copy(land.at[i, t + k], land.at[i, t + k], recv_sem.at[i, t + k]).wait()
        finish(i, source_of(i), t, count, lambda u: land[i, u])

    groups = tiles // GROUP

    @pl.loop(0, EARLY * groups)
    def _(k):
        step(k // groups, lax.rem(k, groups) * GROUP, GROUP)

    for dx in range(1, chips):
        recv_pick(dx).wait_recv()
    for j in range(chips):
        picked[:, j * pair:(j + 1) * pair] = pick[j]

    late = n - 1 - EARLY

    @pl.loop(0, late * (groups - 1))
    def _(k):
        step(EARLY + lax.rem(k, late), (k // late) * GROUP, GROUP)

    @pl.loop(0, late * GROUP)
    def _(k):
        step(EARLY + lax.rem(k, late), tiles - GROUP + k // late, 1)

    pltpu.make_async_copy(land, land, send_sem).wait()
    for i in range(n - 1):
        send_stat(i).wait_send()
    for dx in range(1, chips):
        send_pick(dx).wait_send()


def write_out(table, picked, table_hbm, picked_hbm, sem):
    rows = table.shape[0]
    parts = rows // 8
    copies = [pltpu.make_async_copy(picked, picked_hbm, sem.at[parts])]
    for k in range(parts):
        copies.append(pltpu.make_async_copy(table.at[pl.ds(k * 8, 8), :], table_hbm.at[pl.ds(k * 8, 8), :], sem.at[k]))
    for copy in copies:
        copy.start()
    for copy in copies:
        copy.wait()


def solution(mesh):
    n = mesh.shape["vp"]
    chips = n // 2

    def local_step(hidden, w_local, inv_temp, target_ids):
        batch, depth = hidden.shape
        vocab = w_local.shape[1]
        tiles = vocab // TILE
        own = batch // n
        hbm = pl.BlockSpec(memory_space=pltpu.HBM)
        vmem = pl.BlockSpec(memory_space=pltpu.VMEM)
        dma = pltpu.SemaphoreType.DMA
        table, picked = pl.pallas_call(
            functools.partial(kernel, chips),
            out_shape=(pltpu.VMEM((own, n * vocab), F32), pltpu.VMEM((1, batch), F32)),
            in_specs=[hbm] * 4,
            out_specs=(vmem, vmem),
            scratch_shapes=[
                pltpu.VMEM((batch, depth), BF16),
                pltpu.VMEM((2, depth, TILE), BF16),
                pltpu.VMEM((tiles, batch, TILE), F32),
                pltpu.VMEM((n - 1, tiles, own, TILE), F32),
                pltpu.VMEM((1, batch), F32),
                pltpu.VMEM((1, batch), jnp.int32),
                pltpu.VMEM((batch, LANES), F32),
                pltpu.VMEM((batch, LANES), jnp.int32),
                pltpu.VMEM((batch, LANES), F32),
                pltpu.VMEM((chips, 4, 2 * own), F32),
                pltpu.VMEM((n, 4, 2 * own), F32),
                pltpu.VMEM((chips, 1, 2 * own), F32),
                pltpu.VMEM((2 * own, LANES), F32),
                pltpu.VMEM((own, TILE), F32),
                pltpu.VMEM((own, TILE), F32),
                pltpu.VMEM((n, own, TILE), F32),
                pltpu.VMEM((TILE, TILE), BF16),
                dma((chips,)), dma((2,)), dma((2, PIECES)), dma((2,)), dma, dma((n - 1, tiles)), dma((n - 1,)),
                dma((n - 1,)), dma((chips,)), dma((chips,)),
            ],
            compiler_params=pltpu.CompilerParams(
                collective_id=0, has_side_effects=True, vmem_limit_bytes=52 * 2**20),
        )(hidden, w_local, inv_temp.reshape(1, batch), target_ids.reshape(1, batch))
        table, picked = pl.pallas_call(
            write_out,
            out_shape=(pltpu.HBM(table.shape, F32), pltpu.HBM(picked.shape, F32)),
            in_specs=[vmem] * 2,
            out_specs=(hbm, hbm),
            scratch_shapes=[dma((own // 8 + 1,))],
            compiler_params=pltpu.CompilerParams(vmem_limit_bytes=2**20),
        )(table, picked)
        return table, picked.reshape(batch)

    return jax.shard_map(
        local_step,
        mesh=mesh,
        in_specs=(P("dp", None), P(None, "vp"), P("dp"), P("dp")),
        out_specs=(P(("dp", "vp"), None), P("dp")),
        check_vma=False,
    )
```

```python
import functools

import jax
import jax.numpy as jnp
from jax import lax
from jax.experimental import pallas as pl
from jax.experimental.pallas import tpu as pltpu
from jax.sharding import PartitionSpec as P

MESH = pl.DeviceIdType.MESH
F32 = jnp.float32
BF16 = jnp.bfloat16
TILE = 256
LANES = 128
GROUP = 4
WAITS = (8, 4, 2, 1, 1)
PIECES = 4
PEERS = ((2, 0), (2, 1), (1, 0), (3, 0), (1, 1), (3, 1), (0, 1))
CHIP_ORDER = (2, 1, 3, 0)


def kernel(chips, h_hbm, w_hbm, temp_hbm, ids_hbm, table, picked,
           h, w, z, land, temp_row, ids_row, temp, ids, peak, stat_out, stats, pick, cols, inv_s, top, carry, tri,
           h_sem, w_sem, first_sem, row_sem, send_sem, recv_sem, near_sem, stat_send, stat_recv, pick_send, pick_recv):
    n = 2 * chips
    me = lax.axis_index("vp")
    x, c = me // 2, me % 2
    batch, depth = h_hbm.shape
    vocab = w_hbm.shape[1]
    tiles = vocab // TILE
    own = batch // n
    pair = 2 * own
    piece = depth // PIECES
    remote_peers = n - 2
    firsts = [sum(WAITS[:k]) for k in range(len(WAITS))]

    def peer(i):
        dx, dc = PEERS[i]
        return lax.rem(x + dx, chips) * 2 + lax.rem(c + dc, 2)

    def source(i):
        dx, dc = PEERS[i]
        return lax.rem(x + chips - dx, chips) * 2 + lax.rem(c + dc, 2)

    def held(dx):
        return CHIP_ORDER.index(dx) * pair

    def peer_rows(i):
        dx, dc = PEERS[i]
        return pl.ds(pl.multiple_of(held(dx) + lax.rem(c + dc, 2) * own, own), own)

    def whole_rows(j):
        return pl.ds(pl.multiple_of(lax.rem(x + CHIP_ORDER[j], chips) * pair, pair), pair)

    def h_copy(j):
        return pltpu.make_async_copy(h_hbm.at[whole_rows(j), :], h.at[j * pair:(j + 1) * pair, :], h_sem.at[j])

    def turned(row):
        parts = [row[:, whole_rows(j)] for j in range(chips)]
        return jnp.broadcast_to(jnp.concatenate(parts, axis=1), (LANES, batch)).T

    def w_copy(t):
        col = pl.multiple_of(lax.rem(t, tiles) * TILE, TILE)
        slot = lax.rem(t, 2)
        return pltpu.make_async_copy(w_hbm.at[:, pl.ds(col, TILE)], w.at[slot], w_sem.at[slot])

    def first_copies(k):
        ks = slice(k * piece, (k + 1) * piece)
        return (pltpu.make_async_copy(w_hbm.at[ks, :LANES], w.at[0, ks, :LANES], first_sem.at[0, k]),
                pltpu.make_async_copy(h_hbm.at[whole_rows(0), ks], h.at[:pair, ks], first_sem.at[1, k]))

    second_copy = pltpu.make_async_copy(w_hbm.at[:, LANES:TILE], w.at[0, :, LANES:], w_sem.at[0])

    def remote(src, dst, send, recv, to):
        return pltpu.make_async_remote_copy(
            src_ref=src, dst_ref=dst, send_sem=send, recv_sem=recv, device_id={"vp": to}, device_id_type=MESH)

    def counter(t):
        k = 0
        for first in firsts[1:]:
            k = k + jnp.where(t >= first, 1, 0)
        return k

    def arrival(i, t):
        return near_sem if i == remote_peers else recv_sem.at[i, counter(t)]

    def send(i, t):
        return remote(z.at[t, peer_rows(i), :], land.at[i, t], send_sem, arrival(i, t), peer(i))

    def send_tile(t):
        for i in range(remote_peers):
            send(i, t).start()

    def send_half(i, half):
        ls = slice(half * LANES, (half + 1) * LANES)
        return remote(z.at[0, peer_rows(i), ls], land.at[i, 0, :, ls], send_sem, arrival(i, 0), peer(i))

    def send_stat(i):
        at = stat_out.at[CHIP_ORDER.index(PEERS[i][0])]
        return remote(at, stats.at[me], stat_send, stat_recv, peer(i))

    def send_pick(dx):
        to = lax.rem(x + dx, chips) * 2 + c
        return remote(pick.at[x], pick.at[x], pick_send, pick_recv, to)

    def counted(ref, sem):
        pltpu.make_async_copy(ref, ref, sem).wait()

    barrier = pltpu.get_barrier_semaphore()
    for i in range(n - 1):
        pl.semaphore_signal(barrier, inc=1, device_id={"vp": peer(i)}, device_id_type=MESH)
    temp_copy = pltpu.make_async_copy(temp_hbm, temp_row, row_sem.at[0])
    ids_copy = pltpu.make_async_copy(ids_hbm, ids_row, row_sem.at[1])
    temp_copy.start()
    for k in range(PIECES):
        for copy in first_copies(k):
            copy.start()
    second_copy.start()
    for j in (1, 2):
        h_copy(j).start()
    temp_copy.wait()
    temp[...] = turned(temp_row)

    acc = jnp.zeros((pair, LANES), F32)
    for k in range(PIECES):
        for copy in first_copies(k):
            copy.wait()
        ks = slice(k * piece, (k + 1) * piece)
        acc = acc + jnp.dot(h[:pair, ks], w[0, ks, :LANES], preferred_element_type=F32)
    acc = acc * temp[:pair, :]
    z[0, :pair, :LANES] = acc
    peak[:pair, :] = acc
    pl.semaphore_wait(barrier, n - 1)
    for i in range(2):
        send_half(i, 0).start()
    w_copy(1).start()
    h_copy(3).start()
    ids_copy.start()
    second_copy.wait()
    acc = jnp.dot(h[:pair, :], w[0, :, LANES:], preferred_element_type=F32) * temp[:pair, :]
    z[0, :pair, LANES:] = acc
    peak[:pair, :] = jnp.maximum(peak[:pair, :], acc)
    for i in range(2):
        send_half(i, 1).start()

    def tile_rows(t, slot, rs):
        acc = jnp.dot(h[rs, :], w[slot], preferred_element_type=F32)
        by = temp[rs, :]
        left, right = acc[:, :LANES] * by, acc[:, LANES:] * by
        z[t, rs, :LANES] = left
        z[t, rs, LANES:] = right
        return jnp.maximum(left, right)

    h_copy(1).wait()
    h_copy(2).wait()
    near = pl.ds(pair, 2 * pair)
    peak[near, :] = tile_rows(0, 0, near)
    for i in range(2, remote_peers):
        send(i, 0).start()
    here = pl.ds(3 * pair, pair)
    peak[here, :] = jnp.full((pair, LANES), -jnp.inf, F32)
    h_copy(3).wait()

    @pl.loop(1, tiles)
    def _(t):
        w_copy(t + 1).start()
        w_copy(t).wait()
        best = tile_rows(t, lax.rem(t, 2), pl.ds(0, batch))
        send(remote_peers, t).start()

        @pl.when(lax.rem(t, 2) == 1)
        def _():
            send_tile((t + 1) // 2)
        peak[...] = jnp.maximum(peak[...], best)

    w_copy(tiles).wait()
    peak[here, :] = jnp.maximum(peak[here, :], tile_rows(0, 0, here))
    send(remote_peers, 0).start()

    ids_copy.wait()
    ids[...] = turned(ids_row)
    lane = lax.broadcasted_iota(jnp.int32, (own, LANES), 1)

    @pl.loop(0, n)
    def _(b):
        rs = pl.ds(pl.multiple_of(b * own, own), own)
        most = jnp.broadcast_to(jnp.max(peak[rs, :], axis=1, keepdims=True), (own, LANES))
        target = ids[rs, :] - (me * vocab) - lane

        def add(t, sums):
            total, below = sums
            for half in range(2):
                e = jnp.exp(z[t, rs, half * LANES:(half + 1) * LANES] - most)
                total = total + e
                below = below + jnp.where(target >= t * TILE + half * LANES, e, 0.0)
            return total, below

        zero = jnp.zeros((own, LANES), F32)
        total, below = lax.fori_loop(0, tiles, add, (zero, zero))
        total = jnp.sum(total, axis=1, keepdims=True)
        below = jnp.sum(below, axis=1, keepdims=True)
        peak[rs, :] = jnp.where(lane == 0, most, jnp.where(lane == 1, total, below))

    flipped = peak[...].T
    for j in range(chips):
        stat_out[j] = flipped[:4, j * pair:(j + 1) * pair]
    stats[me] = stat_out[CHIP_ORDER.index(0)]
    for i in range(n - 1):
        send_stat(i).start()

    sent = tiles // 2 + 1
    pl.loop(sent, sent + 3)(send_tile)
    row_id = lax.broadcasted_iota(jnp.int32, (TILE, TILE), 0)
    col_id = lax.broadcasted_iota(jnp.int32, (TILE, TILE), 1)
    tri[...] = jnp.where(row_id <= col_id, 1.0, 0.0).astype(BF16)
    counted(stats.at[pl.ds(0, n - 1)], stat_recv)

    most = stats[0, 0:1, :]
    for d in range(1, n):
        most = jnp.maximum(most, stats[d, 0:1, :])
    mass = jnp.zeros_like(most)
    below = jnp.zeros_like(most)
    lower = []
    for d in range(n):
        lower.append(mass)
        scale = jnp.exp(stats[d, 0:1, :] - most)
        mass = mass + stats[d, 1:2, :] * scale
        below = below + stats[d, 2:3, :] * scale
    pick[x] = below / mass
    for dx in range(1, chips):
        send_pick(dx).start()
    pl.loop(sent + 3, tiles)(send_tile)

    mine = jnp.concatenate(lower + [most, mass, jnp.zeros((LANES - n - 2, pair), F32)], axis=0)
    cols[...] = mine.T
    mine = cols[pl.ds(pl.multiple_of(c * own, own), own), :]
    top[...] = jnp.broadcast_to(mine[:, n:n + 1], (own, TILE))
    scale = 1.0 / jnp.broadcast_to(mine[:, n + 1:n + 2], (own, TILE))
    inv_s[...] = scale
    for i in range(n):
        d = source(i) if i < n - 1 else me
        start = jnp.sum(jnp.where(lane == d, mine, 0.0), axis=1, keepdims=True)
        carry[i] = jnp.broadcast_to(start, (own, TILE)) * scale

    def finish(i, d, t, count, read):
        e = jnp.concatenate([jnp.exp(read(t + k) - top[...]) * inv_s[...] for k in range(count)], axis=0)
        hi = e.astype(BF16)
        rest = e - hi.astype(F32)
        mid = rest.astype(BF16)
        low = (rest - mid.astype(F32)).astype(BF16)
        run = jnp.dot(hi, tri[...], preferred_element_type=F32)
        run = run + jnp.dot(mid, tri[...], preferred_element_type=F32)
        run = run + jnp.dot(low, tri[...], preferred_element_type=F32)
        base = carry[i]
        for k in range(count):
            part = run[k * own:(k + 1) * own, :]
            col = pl.multiple_of(d * vocab + (t + k) * TILE, TILE)
            table[:, pl.ds(col, TILE)] = part + base
            base = base + jnp.broadcast_to(part[:, TILE - 1:], (own, TILE))
        carry[i] = base

    my_rows = pl.ds(pl.multiple_of(held(0) + c * own, own), own)

    @pl.loop(0, tiles // GROUP)
    def _(g):
        finish(n - 1, me, g * GROUP, GROUP, lambda t: z[t, my_rows, :])

    def source_of(i):
        dx = jnp.int32(0)
        dc = jnp.int32(0)
        for k, (kx, kc) in enumerate(PEERS):
            dx = dx + jnp.where(i == k, kx, 0)
            dc = dc + jnp.where(i == k, kc, 0)
        return lax.rem(x + chips - dx, chips) * 2 + lax.rem(c + dc, 2)

    def step(i, t, count):
        finish(i, source_of(i), t, count, lambda u: land[i, u])

    counted(land.at[remote_peers], near_sem)

    @pl.loop(0, tiles // GROUP)
    def _(k):
        step(remote_peers, k * GROUP, GROUP)

    for k, (first, size) in enumerate(zip(firsts, WAITS)):
        if k == len(WAITS) - 1:
            counted(pick.at[pl.ds(0, chips - 1)], pick_recv)
            for j in range(chips):
                picked[:, j * pair:(j + 1) * pair] = pick[j]
        count = min(size, GROUP)
        parts = size // count

        @pl.loop(0, remote_peers * parts)
        def _(u):
            i = lax.rem(u, remote_peers)
            part = u // remote_peers

            @pl.when(part == 0)
            def _():
                counted(land.at[i, pl.ds(first, size)], recv_sem.at[i, k])
            step(i, first + part * count, count)

    counted(land, send_sem)
    counted(stats.at[pl.ds(0, n - 1)], stat_send)
    counted(pick.at[pl.ds(0, chips - 1)], pick_send)


def write_out(table, picked, table_hbm, picked_hbm, sem):
    rows = table.shape[0]
    parts = rows // 8
    copies = [pltpu.make_async_copy(picked, picked_hbm, sem.at[parts])]
    for k in range(parts):
        copies.append(pltpu.make_async_copy(table.at[pl.ds(k * 8, 8), :], table_hbm.at[pl.ds(k * 8, 8), :], sem.at[k]))
    for copy in copies:
        copy.start()
    for copy in copies:
        copy.wait()


def solution(mesh):
    n = mesh.shape["vp"]
    chips = n // 2

    def local_step(hidden, w_local, inv_temp, target_ids):
        batch, depth = hidden.shape
        vocab = w_local.shape[1]
        tiles = vocab // TILE
        own = batch // n
        hbm = pl.BlockSpec(memory_space=pltpu.HBM)
        vmem = pl.BlockSpec(memory_space=pltpu.VMEM)
        dma = pltpu.SemaphoreType.DMA
        table, picked = pl.pallas_call(
            functools.partial(kernel, chips),
            out_shape=(pltpu.VMEM((own, n * vocab), F32), pltpu.VMEM((1, batch), F32)),
            in_specs=[hbm] * 4,
            out_specs=(vmem, vmem),
            scratch_shapes=[
                pltpu.VMEM((batch, depth), BF16),
                pltpu.VMEM((2, depth, TILE), BF16),
                pltpu.VMEM((tiles, batch, TILE), F32),
                pltpu.VMEM((n - 1, tiles, own, TILE), F32),
                pltpu.VMEM((1, batch), F32),
                pltpu.VMEM((1, batch), jnp.int32),
                pltpu.VMEM((batch, LANES), F32),
                pltpu.VMEM((batch, LANES), jnp.int32),
                pltpu.VMEM((batch, LANES), F32),
                pltpu.VMEM((chips, 4, 2 * own), F32),
                pltpu.VMEM((n, 4, 2 * own), F32),
                pltpu.VMEM((chips, 1, 2 * own), F32),
                pltpu.VMEM((2 * own, LANES), F32),
                pltpu.VMEM((own, TILE), F32),
                pltpu.VMEM((own, TILE), F32),
                pltpu.VMEM((n, own, TILE), F32),
                pltpu.VMEM((TILE, TILE), BF16),
                dma((chips,)), dma((2,)), dma((2, PIECES)), dma((2,)), dma, dma((n - 2, len(WAITS))), dma,
                dma, dma, dma, dma,
            ],
            compiler_params=pltpu.CompilerParams(
                collective_id=0, has_side_effects=True, vmem_limit_bytes=52 * 2**20),
        )(hidden, w_local, inv_temp.reshape(1, batch), target_ids.reshape(1, batch))
        table, picked = pl.pallas_call(
            write_out,
            out_shape=(pltpu.HBM(table.shape, F32), pltpu.HBM(picked.shape, F32)),
            in_specs=[vmem] * 2,
            out_specs=(hbm, hbm),
            scratch_shapes=[dma((own // 8 + 1,))],
            compiler_params=pltpu.CompilerParams(vmem_limit_bytes=2**20),
        )(table, picked)
        return table, picked.reshape(batch)

    return jax.shard_map(
        local_step,
        mesh=mesh,
        in_specs=(P("dp", None), P(None, "vp"), P("dp"), P("dp")),
        out_specs=(P(("dp", "vp"), None), P("dp")),
        check_vma=False,
    )
```

```python
import functools

import jax
import jax.numpy as jnp
from jax import lax
from jax.experimental import pallas as pl
from jax.experimental.pallas import tpu as pltpu
from jax.sharding import PartitionSpec as P

MESH = pl.DeviceIdType.MESH
F32 = jnp.float32
BF16 = jnp.bfloat16
TILE = 256
LANES = 128
GROUP = 4
WAITS = (8, 7, 1)
PEERS = ((2, 0), (2, 1), (1, 0), (3, 0), (1, 1), (3, 1), (0, 1))
CHIP_ORDER = (2, 1, 3, 0)


def peer_of(chips, x, c, i):
    dx, dc = PEERS[i]
    return lax.rem(x + dx, chips) * 2 + lax.rem(c + dc, 2)


def source_of(chips, x, c, i):
    dx, dc = PEERS[i]
    return lax.rem(x + chips - dx, chips) * 2 + lax.rem(c + dc, 2)


def triangle():
    row_id = lax.broadcasted_iota(jnp.int32, (TILE, TILE), 0)
    col_id = lax.broadcasted_iota(jnp.int32, (TILE, TILE), 1)
    return jnp.where(row_id <= col_id, 1.0, 0.0).astype(BF16)


def running_sum(e, tri):
    hi = e.astype(BF16)
    rest = e - hi.astype(F32)
    mid = rest.astype(BF16)
    low = (rest - mid.astype(F32)).astype(BF16)
    run = jnp.dot(hi, tri, preferred_element_type=F32)
    run = run + jnp.dot(mid, tri, preferred_element_type=F32)
    return run + jnp.dot(low, tri, preferred_element_type=F32)


def kernel(chips, h_hbm, w_hbm, temp_hbm, ids_hbm, table, picked, last, top, inv_s, carry,
           h, w, z, land, temp_row, ids_row, temp, ids, peak, stat_out, stats, pick, cols, tri,
           h_sem, w_sem, row_sem, send_sem, recv_sem, near_sem, stat_send, stat_recv, pick_send, pick_recv):
    n = 2 * chips
    me = lax.axis_index("vp")
    x, c = me // 2, me % 2
    batch, depth = h_hbm.shape
    vocab = w_hbm.shape[1]
    tiles = vocab // TILE
    own = batch // n
    pair = 2 * own
    remote_peers = n - 2
    firsts = [sum(WAITS[:k]) for k in range(len(WAITS))]

    def peer(i):
        return peer_of(chips, x, c, i)

    def source(i):
        return source_of(chips, x, c, i)

    def held(dx):
        return CHIP_ORDER.index(dx) * pair

    def peer_rows(i):
        dx, dc = PEERS[i]
        return pl.ds(pl.multiple_of(held(dx) + lax.rem(c + dc, 2) * own, own), own)

    def whole_rows(j):
        return pl.ds(pl.multiple_of(lax.rem(x + CHIP_ORDER[j], chips) * pair, pair), pair)

    def h_copy(j):
        return pltpu.make_async_copy(h_hbm.at[whole_rows(j), :], h.at[j * pair:(j + 1) * pair, :], h_sem.at[j])

    def turned(row):
        parts = [row[:, whole_rows(j)] for j in range(chips)]
        return jnp.broadcast_to(jnp.concatenate(parts, axis=1), (LANES, batch)).T

    def w_copy(t):
        col = pl.multiple_of(lax.rem(t, tiles) * TILE, TILE)
        slot = lax.rem(t, 2)
        return pltpu.make_async_copy(w_hbm.at[:, pl.ds(col, TILE)], w.at[slot], w_sem.at[slot])

    first_w = pltpu.make_async_copy(w_hbm.at[:, :LANES], w.at[0, :, :LANES], w_sem.at[1])
    first_h = h_copy(0)
    second_w = pltpu.make_async_copy(w_hbm.at[:, LANES:TILE], w.at[0, :, LANES:], w_sem.at[0])

    def remote(src, dst, send, recv, to):
        return pltpu.make_async_remote_copy(
            src_ref=src, dst_ref=dst, send_sem=send, recv_sem=recv, device_id={"vp": to}, device_id_type=MESH)

    def counter(t):
        k = 0
        for first in firsts[1:]:
            k = k + jnp.where(t >= first, 1, 0)
        return k

    def arrival(i, t):
        return near_sem if i == remote_peers else recv_sem.at[i, counter(t)]

    def send(i, t):
        return remote(z.at[t, peer_rows(i), :], land.at[i, t], send_sem, arrival(i, t), peer(i))

    def send_last(i):
        return remote(z.at[tiles - 1, peer_rows(i), :], last.at[i], send_sem, arrival(i, tiles - 1), peer(i))

    def send_tile(t):
        for i in range(remote_peers):
            send(i, t).start()

    def send_half(i, half):
        ls = slice(half * LANES, (half + 1) * LANES)
        return remote(z.at[0, peer_rows(i), ls], land.at[i, 0, :, ls], send_sem, arrival(i, 0), peer(i))

    def send_stat(i):
        at = stat_out.at[CHIP_ORDER.index(PEERS[i][0])]
        return remote(at, stats.at[me], stat_send, stat_recv, peer(i))

    def send_pick(dx):
        to = lax.rem(x + dx, chips) * 2 + c
        return remote(pick.at[x], pick.at[x], pick_send, pick_recv, to)

    def counted(ref, sem):
        pltpu.make_async_copy(ref, ref, sem).wait()

    temp_copy = pltpu.make_async_copy(temp_hbm, temp_row, row_sem.at[0])
    ids_copy = pltpu.make_async_copy(ids_hbm, ids_row, row_sem.at[1])
    first_w.start()
    first_h.start()
    temp_copy.start()
    barrier = pltpu.get_barrier_semaphore()
    for i in range(n - 1):
        pl.semaphore_signal(barrier, inc=1, device_id={"vp": peer(i)}, device_id_type=MESH)
    second_w.start()
    for j in (1, 2):
        h_copy(j).start()
    temp_copy.wait()
    temp[...] = turned(temp_row)

    first_w.wait()
    first_h.wait()
    acc = jnp.dot(h[:pair, :], w[0, :, :LANES], preferred_element_type=F32) * temp[:pair, :]
    z[0, :pair, :LANES] = acc
    peak[:pair, :] = acc
    pl.semaphore_wait(barrier, n - 1)
    for i in range(2):
        send_half(i, 0).start()
    w_copy(1).start()
    h_copy(3).start()
    ids_copy.start()
    second_w.wait()
    acc = jnp.dot(h[:pair, :], w[0, :, LANES:], preferred_element_type=F32) * temp[:pair, :]
    z[0, :pair, LANES:] = acc
    peak[:pair, :] = jnp.maximum(peak[:pair, :], acc)
    for i in range(2):
        send_half(i, 1).start()

    def tile_rows(t, slot, rs):
        acc = jnp.dot(h[rs, :], w[slot], preferred_element_type=F32)
        by = temp[rs, :]
        left, right = acc[:, :LANES] * by, acc[:, LANES:] * by
        z[t, rs, :LANES] = left
        z[t, rs, LANES:] = right
        return jnp.maximum(left, right)

    h_copy(1).wait()
    h_copy(2).wait()
    near = pl.ds(pair, 2 * pair)
    peak[near, :] = tile_rows(0, 0, near)
    for i in range(2, remote_peers):
        send(i, 0).start()
    here = pl.ds(3 * pair, pair)
    peak[here, :] = jnp.full((pair, LANES), -jnp.inf, F32)
    h_copy(3).wait()

    @pl.loop(1, tiles)
    def _(t):
        w_copy(t + 1).start()
        w_copy(t).wait()
        best = tile_rows(t, lax.rem(t, 2), pl.ds(0, batch))
        send(remote_peers, t).start()

        @pl.when(lax.rem(t, 2) == 1)
        def _():
            send_tile((t + 1) // 2)
        peak[...] = jnp.maximum(peak[...], best)

    w_copy(tiles).wait()
    peak[here, :] = jnp.maximum(peak[here, :], tile_rows(0, 0, here))
    send(remote_peers, 0).start()

    ids_copy.wait()
    ids[...] = turned(ids_row)
    lane = lax.broadcasted_iota(jnp.int32, (own, LANES), 1)

    @pl.loop(0, n)
    def _(b):
        rs = pl.ds(pl.multiple_of(b * own, own), own)
        most = jnp.broadcast_to(jnp.max(peak[rs, :], axis=1, keepdims=True), (own, LANES))
        target = ids[rs, :] - (me * vocab) - lane

        def add(t, sums):
            total, below = sums
            for half in range(2):
                e = jnp.exp(z[t, rs, half * LANES:(half + 1) * LANES] - most)
                total = total + e
                below = below + jnp.where(target >= t * TILE + half * LANES, e, 0.0)
            return total, below

        zero = jnp.zeros((own, LANES), F32)
        total, below = lax.fori_loop(0, tiles, add, (zero, zero))
        total = jnp.sum(total, axis=1, keepdims=True)
        below = jnp.sum(below, axis=1, keepdims=True)
        peak[rs, :] = jnp.where(lane == 0, most, jnp.where(lane == 1, total, below))

    flipped = peak[...].T
    for j in range(chips):
        stat_out[j] = flipped[:4, j * pair:(j + 1) * pair]
    stats[me] = stat_out[CHIP_ORDER.index(0)]
    for i in range(n - 1):
        send_stat(i).start()

    sent = tiles // 2 + 1
    pl.loop(sent, sent + 3)(send_tile)
    tri[...] = triangle()
    counted(stats.at[pl.ds(0, n - 1)], stat_recv)

    most = stats[0, 0:1, :]
    for d in range(1, n):
        most = jnp.maximum(most, stats[d, 0:1, :])
    mass = jnp.zeros_like(most)
    below = jnp.zeros_like(most)
    lower = []
    for d in range(n):
        lower.append(mass)
        scale = jnp.exp(stats[d, 0:1, :] - most)
        mass = mass + stats[d, 1:2, :] * scale
        below = below + stats[d, 2:3, :] * scale
    pick[x] = below / mass
    for dx in range(1, chips):
        send_pick(dx).start()
    pl.loop(sent + 3, tiles - 1)(send_tile)
    for i in range(remote_peers):
        send_last(i).start()

    mine = jnp.concatenate(lower + [most, mass, jnp.zeros((LANES - n - 2, pair), F32)], axis=0)
    cols[...] = mine.T
    mine = cols[pl.ds(pl.multiple_of(c * own, own), own), :]
    top[...] = jnp.broadcast_to(mine[:, n:n + 1], (own, TILE))
    scale = 1.0 / jnp.broadcast_to(mine[:, n + 1:n + 2], (own, TILE))
    inv_s[...] = scale
    for i in range(n):
        d = source(i) if i < n - 1 else me
        start = jnp.sum(jnp.where(lane == d, mine, 0.0), axis=1, keepdims=True)
        carry[i] = jnp.broadcast_to(start, (own, TILE)) * scale

    def finish(i, d, t, count, read):
        e = jnp.concatenate([jnp.exp(read(t + k) - top[...]) * inv_s[...] for k in range(count)], axis=0)
        run = running_sum(e, tri[...])
        base = carry[i]
        for k in range(count):
            part = run[k * own:(k + 1) * own, :]
            col = pl.multiple_of(d * vocab + (t + k) * TILE, TILE)
            table[:, pl.ds(col, TILE)] = part + base
            base = base + jnp.broadcast_to(part[:, TILE - 1:], (own, TILE))
        carry[i] = base

    my_rows = pl.ds(pl.multiple_of(held(0) + c * own, own), own)

    @pl.loop(0, tiles // GROUP)
    def _(g):
        finish(n - 1, me, g * GROUP, GROUP, lambda t: z[t, my_rows, :])

    def source_at(i):
        d = jnp.int32(0)
        for k in range(n - 1):
            d = d + jnp.where(i == k, source(k), 0)
        return d

    def step(i, t, count):
        finish(i, source_at(i), t, count, lambda u: land[i, u])

    counted(land.at[remote_peers], near_sem)

    @pl.loop(0, tiles // GROUP)
    def _(k):
        step(remote_peers, k * GROUP, GROUP)

    for k in range(len(WAITS) - 1):
        first, size = firsts[k], WAITS[k]
        count = min(size, 2 * GROUP - 1) if size % GROUP else GROUP
        parts = size // count

        @pl.loop(0, remote_peers * parts)
        def _(u):
            i = lax.rem(u, remote_peers)
            part = u // remote_peers

            @pl.when(part == 0)
            def _():
                counted(land.at[i, pl.ds(first, size)], recv_sem.at[i, k])
            step(i, first + part * count, count)

    counted(pick.at[pl.ds(0, chips - 1)], pick_recv)
    for j in range(chips):
        picked[:, j * pair:(j + 1) * pair] = pick[j]
    for i in range(remote_peers):
        counted(last.at[i], recv_sem.at[i, len(WAITS) - 1])
    counted(land, send_sem)
    counted(stats.at[pl.ds(0, n - 1)], stat_send)
    counted(pick.at[pl.ds(0, chips - 1)], pick_send)


def write_out(chips, table, picked, last, top, inv_s, carry, table_hbm, picked_hbm, done, sem):
    n = 2 * chips
    me = lax.axis_index("vp")
    x, c = me // 2, me % 2
    own, width = table.shape
    vocab = width // n
    bulk = vocab - TILE

    def put(d, first, size, sem, source=None):
        cs = pl.ds(pl.multiple_of(d * vocab + first, TILE), size)
        return pltpu.make_async_copy(table.at[:, cs] if source is None else source, table_hbm.at[:, cs], sem)

    for d in range(n):
        put(d, 0, bulk, sem.at[0]).start()
    for d in (me, source_of(chips, x, c, n - 2)):
        put(d, bulk, TILE, sem.at[1]).start()
    picked_copy = pltpu.make_async_copy(picked, picked_hbm, sem.at[2])
    picked_copy.start()
    e = jnp.concatenate([jnp.exp(last[i] - top[...]) * inv_s[...] for i in range(n - 2)], axis=0)
    run = running_sum(e, triangle())
    for i in range(n - 2):
        done[i] = run[i * own:(i + 1) * own, :] + carry[i]
    for i in range(n - 2):
        put(source_of(chips, x, c, i), bulk, TILE, sem.at[1], done.at[i]).start()
    picked_copy.wait()
    put(0, 0, n * bulk, sem.at[0]).wait()
    put(0, 0, n * TILE, sem.at[1]).wait()


def solution(mesh):
    n = mesh.shape["vp"]
    chips = n // 2

    def local_step(hidden, w_local, inv_temp, target_ids):
        batch, depth = hidden.shape
        vocab = w_local.shape[1]
        tiles = vocab // TILE
        own = batch // n
        hbm = pl.BlockSpec(memory_space=pltpu.HBM)
        vmem = pl.BlockSpec(memory_space=pltpu.VMEM)
        dma = pltpu.SemaphoreType.DMA
        out = (pltpu.VMEM((own, n * vocab), F32), pltpu.VMEM((1, batch), F32), pltpu.VMEM((n - 2, own, TILE), F32),
               pltpu.VMEM((own, TILE), F32), pltpu.VMEM((own, TILE), F32), pltpu.VMEM((n, own, TILE), F32))
        parts = pl.pallas_call(
            functools.partial(kernel, chips),
            out_shape=out,
            in_specs=[hbm] * 4,
            out_specs=(vmem,) * len(out),
            scratch_shapes=[
                pltpu.VMEM((batch, depth), BF16),
                pltpu.VMEM((2, depth, TILE), BF16),
                pltpu.VMEM((tiles, batch, TILE), F32),
                pltpu.VMEM((n - 1, tiles, own, TILE), F32),
                pltpu.VMEM((1, batch), F32),
                pltpu.VMEM((1, batch), jnp.int32),
                pltpu.VMEM((batch, LANES), F32),
                pltpu.VMEM((batch, LANES), jnp.int32),
                pltpu.VMEM((batch, LANES), F32),
                pltpu.VMEM((chips, 4, 2 * own), F32),
                pltpu.VMEM((n, 4, 2 * own), F32),
                pltpu.VMEM((chips, 1, 2 * own), F32),
                pltpu.VMEM((2 * own, LANES), F32),
                pltpu.VMEM((TILE, TILE), BF16),
                dma((chips,)), dma((2,)), dma((2,)), dma, dma((n - 2, len(WAITS))), dma,
                dma, dma, dma, dma,
            ],
            compiler_params=pltpu.CompilerParams(
                collective_id=0, has_side_effects=True, vmem_limit_bytes=52 * 2**20),
        )(hidden, w_local, inv_temp.reshape(1, batch), target_ids.reshape(1, batch))
        table, picked = pl.pallas_call(
            functools.partial(write_out, chips),
            out_shape=(pltpu.HBM((own, n * vocab), F32), pltpu.HBM((1, batch), F32)),
            in_specs=[vmem] * len(out),
            out_specs=(hbm, hbm),
            scratch_shapes=[pltpu.VMEM((n - 2, own, TILE), F32), dma((3,))],
            compiler_params=pltpu.CompilerParams(vmem_limit_bytes=8 * 2**20),
        )(*parts)
        return table, picked.reshape(batch)

    return jax.shard_map(
        local_step,
        mesh=mesh,
        in_specs=(P("dp", None), P(None, "vp"), P("dp"), P("dp")),
        out_specs=(P(("dp", "vp"), None), P("dp")),
        check_vma=False,
    )
```

```python
import functools

import jax
import jax.numpy as jnp
from jax import lax
from jax.experimental import pallas as pl
from jax.experimental.pallas import tpu as pltpu
from jax.sharding import PartitionSpec as P

MESH = pl.DeviceIdType.MESH
F32 = jnp.float32
BF16 = jnp.bfloat16
TILE = 256
LANES = 128
GROUP = 4
WAITS = (8, 7, 1)
PEERS = ((2, 0), (2, 1), (1, 0), (3, 0), (1, 1), (3, 1), (0, 1))
CHIP_ORDER = (2, 1, 3, 0)


def peer_of(chips, x, c, i):
    dx, dc = PEERS[i]
    return lax.rem(x + dx, chips) * 2 + lax.rem(c + dc, 2)


def source_of(chips, x, c, i):
    dx, dc = PEERS[i]
    return lax.rem(x + chips - dx, chips) * 2 + lax.rem(c + dc, 2)


def triangle():
    row_id = lax.broadcasted_iota(jnp.int32, (TILE, TILE), 0)
    col_id = lax.broadcasted_iota(jnp.int32, (TILE, TILE), 1)
    return jnp.where(row_id <= col_id, 1.0, 0.0).astype(BF16)


def running_sum(e, tri):
    hi = e.astype(BF16)
    rest = e - hi.astype(F32)
    mid = rest.astype(BF16)
    low = (rest - mid.astype(F32)).astype(BF16)
    run = jnp.dot(hi, tri, preferred_element_type=F32)
    run = run + jnp.dot(mid, tri, preferred_element_type=F32)
    return run + jnp.dot(low, tri, preferred_element_type=F32)


def kernel(chips, h_hbm, w_hbm, temp_hbm, ids_hbm, table, picked, last, top, inv_s, carry,
           h, w, z, land, temp_row, ids_row, temp, ids, peak, stat_out, stats, pick, cols, tri,
           h_sem, w_sem, row_sem, send_sem, recv_sem, near_sem, stat_send, stat_recv, pick_send, pick_recv):
    n = 2 * chips
    me = lax.axis_index("vp")
    x, c = me // 2, me % 2
    batch, depth = h_hbm.shape
    vocab = w_hbm.shape[1]
    tiles = vocab // TILE
    own = batch // n
    pair = 2 * own
    remote_peers = n - 2
    firsts = [sum(WAITS[:k]) for k in range(len(WAITS))]

    def peer(i):
        return peer_of(chips, x, c, i)

    def source(i):
        return source_of(chips, x, c, i)

    def held(dx):
        return CHIP_ORDER.index(dx) * pair

    def peer_rows(i):
        dx, dc = PEERS[i]
        return pl.ds(pl.multiple_of(held(dx) + lax.rem(c + dc, 2) * own, own), own)

    def whole_rows(j):
        return pl.ds(pl.multiple_of(lax.rem(x + CHIP_ORDER[j], chips) * pair, pair), pair)

    def h_copy(j):
        return pltpu.make_async_copy(h_hbm.at[whole_rows(j), :], h.at[j * pair:(j + 1) * pair, :], h_sem.at[j])

    def turned(row):
        parts = [row[:, whole_rows(j)] for j in range(chips)]
        return jnp.broadcast_to(jnp.concatenate(parts, axis=1), (LANES, batch)).T

    def w_copy(t):
        col = pl.multiple_of(lax.rem(t, tiles) * TILE, TILE)
        slot = lax.rem(t, 2)
        return pltpu.make_async_copy(w_hbm.at[:, pl.ds(col, TILE)], w.at[slot], w_sem.at[slot])

    first_w = pltpu.make_async_copy(w_hbm.at[:, :LANES], w.at[0, :, :LANES], w_sem.at[1])
    def far_copy(core):
        r = pl.multiple_of((lax.rem(x + 2, chips) * 2 + core) * own, own)
        sem = h_sem.at[chips] if core else h_sem.at[0]
        return pltpu.make_async_copy(h_hbm.at[pl.ds(r, own), :], h.at[core * own:(core + 1) * own, :], sem)

    second_w = pltpu.make_async_copy(w_hbm.at[:, LANES:TILE], w.at[0, :, LANES:], w_sem.at[0])

    def remote(src, dst, send, recv, to):
        return pltpu.make_async_remote_copy(
            src_ref=src, dst_ref=dst, send_sem=send, recv_sem=recv, device_id={"vp": to}, device_id_type=MESH)

    def counter(t):
        k = 0
        for first in firsts[1:]:
            k = k + jnp.where(t >= first, 1, 0)
        return k

    def arrival(i, t):
        return near_sem if i == remote_peers else recv_sem.at[i, counter(t)]

    def send(i, t):
        return remote(z.at[t, peer_rows(i), :], land.at[i, t], send_sem, arrival(i, t), peer(i))

    def send_last(i):
        return remote(z.at[tiles - 1, peer_rows(i), :], last.at[i], send_sem, arrival(i, tiles - 1), peer(i))

    def send_tile(t):
        for i in range(remote_peers):
            send(i, t).start()

    def send_stat(i):
        at = stat_out.at[CHIP_ORDER.index(PEERS[i][0])]
        return remote(at, stats.at[me], stat_send, stat_recv, peer(i))

    def send_pick(dx):
        to = lax.rem(x + dx, chips) * 2 + c
        return remote(pick.at[x], pick.at[x], pick_send, pick_recv, to)

    def counted(ref, sem):
        pltpu.make_async_copy(ref, ref, sem).wait()

    temp_copy = pltpu.make_async_copy(temp_hbm, temp_row, row_sem.at[0])
    ids_copy = pltpu.make_async_copy(ids_hbm, ids_row, row_sem.at[1])
    first_w.start()
    for core in range(2):
        far_copy(core).start()
    temp_copy.start()
    barrier = pltpu.get_barrier_semaphore()
    for i in range(n - 1):
        pl.semaphore_signal(barrier, inc=1, device_id={"vp": peer(i)}, device_id_type=MESH)
    second_w.start()
    for j in (1, 2):
        h_copy(j).start()
    temp_copy.wait()
    temp[...] = turned(temp_row)

    first_w.wait()
    far_copy(0).wait()
    def far_part(core, half):
        rs, ls = slice(core * own, (core + 1) * own), slice(half * LANES, (half + 1) * LANES)
        acc = jnp.dot(h[rs, :], w[0, :, ls], preferred_element_type=F32) * temp[rs, :]
        z[0, rs, ls] = acc
        peak[rs, :] = jnp.maximum(peak[rs, :], acc) if half else acc

    def far_send(core, half):
        ls = slice(half * LANES, (half + 1) * LANES)
        slot = lax.rem(core + c, 2)
        remote(z.at[0, core * own:(core + 1) * own, ls], land.at[slot, 0, :, ls], send_sem, recv_sem.at[slot, 0],
               lax.rem(x + 2, chips) * 2 + core).start()

    far_part(0, 0)
    pl.semaphore_wait(barrier, n - 1)
    far_send(0, 0)
    far_copy(1).wait()
    far_part(1, 0)
    far_send(1, 0)
    w_copy(1).start()
    h_copy(3).start()
    ids_copy.start()
    second_w.wait()
    for core in range(2):
        far_part(core, 1)
        far_send(core, 1)

    def tile_rows(t, slot, rs):
        acc = jnp.dot(h[rs, :], w[slot], preferred_element_type=F32)
        by = temp[rs, :]
        left, right = acc[:, :LANES] * by, acc[:, LANES:] * by
        z[t, rs, :LANES] = left
        z[t, rs, LANES:] = right
        return jnp.maximum(left, right)

    h_copy(1).wait()
    h_copy(2).wait()
    near = pl.ds(pair, 2 * pair)
    peak[near, :] = tile_rows(0, 0, near)
    for i in range(2, remote_peers):
        send(i, 0).start()
    here = pl.ds(3 * pair, pair)
    peak[here, :] = jnp.full((pair, LANES), -jnp.inf, F32)
    h_copy(3).wait()

    @pl.loop(1, tiles)
    def _(t):
        w_copy(t + 1).start()
        w_copy(t).wait()
        best = tile_rows(t, lax.rem(t, 2), pl.ds(0, batch))
        send(remote_peers, t).start()

        @pl.when(lax.rem(t, 2) == 1)
        def _():
            send_tile((t + 1) // 2)
        peak[...] = jnp.maximum(peak[...], best)

    w_copy(tiles).wait()
    peak[here, :] = jnp.maximum(peak[here, :], tile_rows(0, 0, here))
    send(remote_peers, 0).start()

    ids_copy.wait()
    ids[...] = turned(ids_row)
    lane = lax.broadcasted_iota(jnp.int32, (own, LANES), 1)

    @pl.loop(0, n)
    def _(b):
        rs = pl.ds(pl.multiple_of(b * own, own), own)
        most = jnp.broadcast_to(jnp.max(peak[rs, :], axis=1, keepdims=True), (own, LANES))
        target = ids[rs, :] - (me * vocab) - lane

        def add(t, sums):
            total, below = sums
            for half in range(2):
                e = jnp.exp(z[t, rs, half * LANES:(half + 1) * LANES] - most)
                total = total + e
                below = below + jnp.where(target >= t * TILE + half * LANES, e, 0.0)
            return total, below

        zero = jnp.zeros((own, LANES), F32)
        total, below = lax.fori_loop(0, tiles, add, (zero, zero))
        total = jnp.sum(total, axis=1, keepdims=True)
        below = jnp.sum(below, axis=1, keepdims=True)
        peak[rs, :] = jnp.where(lane == 0, most, jnp.where(lane == 1, total, below))

    flipped = peak[...].T
    for j in range(chips):
        stat_out[j] = flipped[:4, j * pair:(j + 1) * pair]
    stats[me] = stat_out[CHIP_ORDER.index(0)]
    for i in range(n - 1):
        send_stat(i).start()

    sent = tiles // 2 + 1
    pl.loop(sent, sent + 3)(send_tile)
    tri[...] = triangle()
    counted(stats.at[pl.ds(0, n - 1)], stat_recv)

    most = stats[0, 0:1, :]
    for d in range(1, n):
        most = jnp.maximum(most, stats[d, 0:1, :])
    mass = jnp.zeros_like(most)
    below = jnp.zeros_like(most)
    lower = []
    for d in range(n):
        lower.append(mass)
        scale = jnp.exp(stats[d, 0:1, :] - most)
        mass = mass + stats[d, 1:2, :] * scale
        below = below + stats[d, 2:3, :] * scale
    pick[x] = below / mass
    for dx in range(1, chips):
        send_pick(dx).start()
    pl.loop(sent + 3, tiles - 1)(send_tile)
    for i in range(remote_peers):
        send_last(i).start()

    mine = jnp.concatenate(lower + [most, mass, jnp.zeros((LANES - n - 2, pair), F32)], axis=0)
    cols[...] = mine.T
    mine = cols[pl.ds(pl.multiple_of(c * own, own), own), :]
    top[...] = jnp.broadcast_to(mine[:, n:n + 1], (own, TILE))
    scale = 1.0 / jnp.broadcast_to(mine[:, n + 1:n + 2], (own, TILE))
    inv_s[...] = scale
    for i in range(n):
        d = source(i) if i < n - 1 else me
        start = jnp.sum(jnp.where(lane == d, mine, 0.0), axis=1, keepdims=True)
        carry[i] = jnp.broadcast_to(start, (own, TILE)) * scale

    def finish(i, d, t, count, read):
        e = jnp.concatenate([jnp.exp(read(t + k) - top[...]) * inv_s[...] for k in range(count)], axis=0)
        run = running_sum(e, tri[...])
        base = carry[i]
        for k in range(count):
            part = run[k * own:(k + 1) * own, :]
            col = pl.multiple_of(d * vocab + (t + k) * TILE, TILE)
            table[:, pl.ds(col, TILE)] = part + base
            base = base + jnp.broadcast_to(part[:, TILE - 1:], (own, TILE))
        carry[i] = base

    my_rows = pl.ds(pl.multiple_of(held(0) + c * own, own), own)

    @pl.loop(0, tiles // GROUP)
    def _(g):
        finish(n - 1, me, g * GROUP, GROUP, lambda t: z[t, my_rows, :])

    def source_at(i):
        d = jnp.int32(0)
        for k in range(n - 1):
            d = d + jnp.where(i == k, source(k), 0)
        return d

    def step(i, t, count):
        finish(i, source_at(i), t, count, lambda u: land[i, u])

    counted(land.at[remote_peers], near_sem)

    @pl.loop(0, tiles // GROUP)
    def _(k):
        step(remote_peers, k * GROUP, GROUP)

    for k in range(len(WAITS) - 1):
        first, size = firsts[k], WAITS[k]
        count = min(size, 2 * GROUP - 1) if size % GROUP else GROUP
        parts = size // count

        @pl.loop(0, remote_peers * parts)
        def _(u):
            i = lax.rem(u, remote_peers)
            part = u // remote_peers

            @pl.when(part == 0)
            def _():
                counted(land.at[i, pl.ds(first, size)], recv_sem.at[i, k])
            step(i, first + part * count, count)

    counted(pick.at[pl.ds(0, chips - 1)], pick_recv)
    for j in range(chips):
        picked[:, j * pair:(j + 1) * pair] = pick[j]
    for i in range(remote_peers):
        counted(last.at[i], recv_sem.at[i, len(WAITS) - 1])
    counted(land, send_sem)
    counted(stats.at[pl.ds(0, n - 1)], stat_send)
    counted(pick.at[pl.ds(0, chips - 1)], pick_send)


def write_out(chips, table, picked, last, top, inv_s, carry, table_hbm, picked_hbm, done, sem):
    n = 2 * chips
    me = lax.axis_index("vp")
    x, c = me // 2, me % 2
    own, width = table.shape
    vocab = width // n
    bulk = vocab - TILE

    def put(d, first, size, sem, source=None):
        cs = pl.ds(pl.multiple_of(d * vocab + first, TILE), size)
        return pltpu.make_async_copy(table.at[:, cs] if source is None else source, table_hbm.at[:, cs], sem)

    for d in range(n):
        put(d, 0, bulk, sem.at[0]).start()
    for d in (me, source_of(chips, x, c, n - 2)):
        put(d, bulk, TILE, sem.at[1]).start()
    picked_copy = pltpu.make_async_copy(picked, picked_hbm, sem.at[2])
    picked_copy.start()
    e = jnp.concatenate([jnp.exp(last[i] - top[...]) * inv_s[...] for i in range(n - 2)], axis=0)
    run = running_sum(e, triangle())
    for i in range(n - 2):
        done[i] = run[i * own:(i + 1) * own, :] + carry[i]
    for i in range(n - 2):
        put(source_of(chips, x, c, i), bulk, TILE, sem.at[1], done.at[i]).start()
    picked_copy.wait()
    put(0, 0, n * bulk, sem.at[0]).wait()
    put(0, 0, n * TILE, sem.at[1]).wait()


def solution(mesh):
    n = mesh.shape["vp"]
    chips = n // 2

    def local_step(hidden, w_local, inv_temp, target_ids):
        batch, depth = hidden.shape
        vocab = w_local.shape[1]
        tiles = vocab // TILE
        own = batch // n
        hbm = pl.BlockSpec(memory_space=pltpu.HBM)
        vmem = pl.BlockSpec(memory_space=pltpu.VMEM)
        dma = pltpu.SemaphoreType.DMA
        out = (pltpu.VMEM((own, n * vocab), F32), pltpu.VMEM((1, batch), F32), pltpu.VMEM((n - 2, own, TILE), F32),
               pltpu.VMEM((own, TILE), F32), pltpu.VMEM((own, TILE), F32), pltpu.VMEM((n, own, TILE), F32))
        parts = pl.pallas_call(
            functools.partial(kernel, chips),
            out_shape=out,
            in_specs=[hbm] * 4,
            out_specs=(vmem,) * len(out),
            scratch_shapes=[
                pltpu.VMEM((batch, depth), BF16),
                pltpu.VMEM((2, depth, TILE), BF16),
                pltpu.VMEM((tiles, batch, TILE), F32),
                pltpu.VMEM((n - 1, tiles, own, TILE), F32),
                pltpu.VMEM((1, batch), F32),
                pltpu.VMEM((1, batch), jnp.int32),
                pltpu.VMEM((batch, LANES), F32),
                pltpu.VMEM((batch, LANES), jnp.int32),
                pltpu.VMEM((batch, LANES), F32),
                pltpu.VMEM((chips, 4, 2 * own), F32),
                pltpu.VMEM((n, 4, 2 * own), F32),
                pltpu.VMEM((chips, 1, 2 * own), F32),
                pltpu.VMEM((2 * own, LANES), F32),
                pltpu.VMEM((TILE, TILE), BF16),
                dma((chips + 1,)), dma((2,)), dma((2,)), dma, dma((n - 2, len(WAITS))), dma,
                dma, dma, dma, dma,
            ],
            compiler_params=pltpu.CompilerParams(
                collective_id=0, has_side_effects=True, vmem_limit_bytes=52 * 2**20),
        )(hidden, w_local, inv_temp.reshape(1, batch), target_ids.reshape(1, batch))
        table, picked = pl.pallas_call(
            functools.partial(write_out, chips),
            out_shape=(pltpu.HBM((own, n * vocab), F32), pltpu.HBM((1, batch), F32)),
            in_specs=[vmem] * len(out),
            out_specs=(hbm, hbm),
            scratch_shapes=[pltpu.VMEM((n - 2, own, TILE), F32), dma((3,))],
            compiler_params=pltpu.CompilerParams(vmem_limit_bytes=8 * 2**20),
        )(*parts)
        return table, picked.reshape(batch)

    return jax.shard_map(
        local_step,
        mesh=mesh,
        in_specs=(P("dp", None), P(None, "vp"), P("dp"), P("dp")),
        out_specs=(P(("dp", "vp"), None), P("dp")),
        check_vma=False,
    )
```

```python
import functools

import jax
import jax.numpy as jnp
from jax import lax
from jax.experimental import pallas as pl
from jax.experimental.pallas import tpu as pltpu
from jax.sharding import PartitionSpec as P

MESH = pl.DeviceIdType.MESH
F32 = jnp.float32
BF16 = jnp.bfloat16
TILE = 256
LANES = 128
GROUP = 4
WAITS = (8, 4, 3, 1)
PEERS = ((2, 0), (2, 1), (1, 0), (3, 0), (1, 1), (3, 1), (0, 1))
CHIP_ORDER = (2, 1, 3, 0)


def peer_of(chips, x, c, i):
    dx, dc = PEERS[i]
    return lax.rem(x + dx, chips) * 2 + lax.rem(c + dc, 2)


def source_of(chips, x, c, i):
    dx, dc = PEERS[i]
    return lax.rem(x + chips - dx, chips) * 2 + lax.rem(c + dc, 2)


def triangle():
    row_id = lax.broadcasted_iota(jnp.int32, (TILE, TILE), 0)
    col_id = lax.broadcasted_iota(jnp.int32, (TILE, TILE), 1)
    return jnp.where(row_id <= col_id, 1.0, 0.0).astype(BF16)


def running_sum(e, tri):
    hi = e.astype(BF16)
    rest = e - hi.astype(F32)
    mid = rest.astype(BF16)
    low = (rest - mid.astype(F32)).astype(BF16)
    run = jnp.dot(hi, tri, preferred_element_type=F32)
    run = run + jnp.dot(mid, tri, preferred_element_type=F32)
    return run + jnp.dot(low, tri, preferred_element_type=F32)


def kernel(chips, h_hbm, w_hbm, temp_hbm, ids_hbm, table, picked, last, top, inv_s, carry,
           h, w, z, land, temp_row, ids_row, temp, ids, peak, stat_out, stats, pick, cols, tri,
           h_sem, w_sem, row_sem, send_sem, recv_sem, near_sem, stat_send, stat_recv, pick_send, pick_recv):
    n = 2 * chips
    me = lax.axis_index("vp")
    x, c = me // 2, me % 2
    batch, depth = h_hbm.shape
    vocab = w_hbm.shape[1]
    tiles = vocab // TILE
    own = batch // n
    pair = 2 * own
    remote_peers = n - 2
    firsts = [sum(WAITS[:k]) for k in range(len(WAITS))]

    def peer(i):
        return peer_of(chips, x, c, i)

    def source(i):
        return source_of(chips, x, c, i)

    def held(dx):
        return CHIP_ORDER.index(dx) * pair

    def peer_rows(i):
        dx, dc = PEERS[i]
        return pl.ds(pl.multiple_of(held(dx) + lax.rem(c + dc, 2) * own, own), own)

    def whole_rows(j):
        return pl.ds(pl.multiple_of(lax.rem(x + CHIP_ORDER[j], chips) * pair, pair), pair)

    def h_copy(j):
        return pltpu.make_async_copy(h_hbm.at[whole_rows(j), :], h.at[j * pair:(j + 1) * pair, :], h_sem.at[j])

    def turned(row):
        parts = [row[:, whole_rows(j)] for j in range(chips)]
        return jnp.broadcast_to(jnp.concatenate(parts, axis=1), (LANES, batch)).T

    def w_copy(t):
        col = pl.multiple_of(lax.rem(t, tiles) * TILE, TILE)
        slot = lax.rem(t, 2)
        return pltpu.make_async_copy(w_hbm.at[:, pl.ds(col, TILE)], w.at[slot], w_sem.at[slot])

    first_w = pltpu.make_async_copy(w_hbm.at[:, :LANES], w.at[0, :, :LANES], w_sem.at[1])
    def far_copy(core):
        r = pl.multiple_of((lax.rem(x + 2, chips) * 2 + core) * own, own)
        sem = h_sem.at[chips] if core else h_sem.at[0]
        return pltpu.make_async_copy(h_hbm.at[pl.ds(r, own), :], h.at[core * own:(core + 1) * own, :], sem)

    second_w = pltpu.make_async_copy(w_hbm.at[:, LANES:TILE], w.at[0, :, LANES:], w_sem.at[0])

    def remote(src, dst, send, recv, to):
        return pltpu.make_async_remote_copy(
            src_ref=src, dst_ref=dst, send_sem=send, recv_sem=recv, device_id={"vp": to}, device_id_type=MESH)

    def counter(t):
        k = 0
        for first in firsts[1:]:
            k = k + jnp.where(t >= first, 1, 0)
        return k

    def arrival(i, t):
        return near_sem if i == remote_peers else recv_sem.at[counter(t)]

    def send(i, t):
        return remote(z.at[t, peer_rows(i), :], land.at[i, t], send_sem, arrival(i, t), peer(i))

    def send_last(i):
        return remote(z.at[tiles - 1, peer_rows(i), :], last.at[i], send_sem, arrival(i, tiles - 1), peer(i))

    def send_tile(t):
        for i in range(remote_peers):
            send(i, t).start()

    def send_stat(i):
        at = stat_out.at[CHIP_ORDER.index(PEERS[i][0])]
        return remote(at, stats.at[me], stat_send, stat_recv, peer(i))

    def send_pick(dx):
        to = lax.rem(x + dx, chips) * 2 + c
        return remote(pick.at[x], pick.at[x], pick_send, pick_recv, to)

    def counted(ref, sem):
        pltpu.make_async_copy(ref, ref, sem).wait()

    temp_copy = pltpu.make_async_copy(temp_hbm, temp_row, row_sem.at[0])
    ids_copy = pltpu.make_async_copy(ids_hbm, ids_row, row_sem.at[1])
    first_w.start()
    for core in range(2):
        far_copy(core).start()
    temp_copy.start()
    barrier = pltpu.get_barrier_semaphore()
    for i in range(n - 1):
        pl.semaphore_signal(barrier, inc=1, device_id={"vp": peer(i)}, device_id_type=MESH)
    second_w.start()
    for j in (1, 2):
        h_copy(j).start()
    temp_copy.wait()
    temp[...] = turned(temp_row)

    first_w.wait()
    far_copy(0).wait()
    def far_part(core, half):
        rs, ls = slice(core * own, (core + 1) * own), slice(half * LANES, (half + 1) * LANES)
        acc = jnp.dot(h[rs, :], w[0, :, ls], preferred_element_type=F32) * temp[rs, :]
        z[0, rs, ls] = acc
        peak[rs, :] = jnp.maximum(peak[rs, :], acc) if half else acc

    def far_send(core, half):
        ls = slice(half * LANES, (half + 1) * LANES)
        slot = lax.rem(core + c, 2)
        remote(z.at[0, core * own:(core + 1) * own, ls], land.at[slot, 0, :, ls], send_sem, recv_sem.at[0],
               lax.rem(x + 2, chips) * 2 + core).start()

    far_part(0, 0)
    pl.semaphore_wait(barrier, n - 1)
    far_send(0, 0)
    far_copy(1).wait()
    far_part(1, 0)
    far_send(1, 0)
    w_copy(1).start()
    h_copy(3).start()
    ids_copy.start()
    second_w.wait()
    for core in range(2):
        far_part(core, 1)
        far_send(core, 1)

    def tile_rows(t, slot, rs):
        acc = jnp.dot(h[rs, :], w[slot], preferred_element_type=F32)
        by = temp[rs, :]
        left, right = acc[:, :LANES] * by, acc[:, LANES:] * by
        z[t, rs, :LANES] = left
        z[t, rs, LANES:] = right
        return jnp.maximum(left, right)

    h_copy(1).wait()
    h_copy(2).wait()
    near = pl.ds(pair, 2 * pair)
    peak[near, :] = tile_rows(0, 0, near)
    for i in range(2, remote_peers):
        send(i, 0).start()
    here = pl.ds(3 * pair, pair)
    peak[here, :] = jnp.full((pair, LANES), -jnp.inf, F32)
    h_copy(3).wait()

    @pl.loop(1, tiles)
    def _(t):
        w_copy(t + 1).start()
        w_copy(t).wait()
        best = tile_rows(t, lax.rem(t, 2), pl.ds(0, batch))
        send(remote_peers, t).start()

        @pl.when(lax.rem(t, 2) == 1)
        def _():
            send_tile((t + 1) // 2)
        peak[...] = jnp.maximum(peak[...], best)

    w_copy(tiles).wait()
    peak[here, :] = jnp.maximum(peak[here, :], tile_rows(0, 0, here))
    send(remote_peers, 0).start()

    ids_copy.wait()
    ids[...] = turned(ids_row)
    lane = lax.broadcasted_iota(jnp.int32, (own, LANES), 1)

    @pl.loop(0, n)
    def _(b):
        rs = pl.ds(pl.multiple_of(b * own, own), own)
        most = jnp.broadcast_to(jnp.max(peak[rs, :], axis=1, keepdims=True), (own, LANES))
        target = ids[rs, :] - (me * vocab) - lane

        def add(t, sums):
            total, below = sums
            for half in range(2):
                e = jnp.exp(z[t, rs, half * LANES:(half + 1) * LANES] - most)
                total = total + e
                below = below + jnp.where(target >= t * TILE + half * LANES, e, 0.0)
            return total, below

        zero = jnp.zeros((own, LANES), F32)
        total, below = lax.fori_loop(0, tiles, add, (zero, zero))
        total = jnp.sum(total, axis=1, keepdims=True)
        below = jnp.sum(below, axis=1, keepdims=True)
        peak[rs, :] = jnp.where(lane == 0, most, jnp.where(lane == 1, total, below))

    flipped = peak[...].T
    for j in range(chips):
        stat_out[j] = flipped[:4, j * pair:(j + 1) * pair]
    stats[me] = stat_out[CHIP_ORDER.index(0)]
    for i in range(n - 1):
        send_stat(i).start()

    sent = tiles // 2 + 1
    pl.loop(sent, sent + 3)(send_tile)
    tri[...] = triangle()
    counted(stats.at[pl.ds(0, n - 1)], stat_recv)

    most = stats[0, 0:1, :]
    for d in range(1, n):
        most = jnp.maximum(most, stats[d, 0:1, :])
    mass = jnp.zeros_like(most)
    below = jnp.zeros_like(most)
    lower = []
    for d in range(n):
        lower.append(mass)
        scale = jnp.exp(stats[d, 0:1, :] - most)
        mass = mass + stats[d, 1:2, :] * scale
        below = below + stats[d, 2:3, :] * scale
    pick[x] = below / mass
    for dx in range(1, chips):
        send_pick(dx).start()
    pl.loop(sent + 3, tiles - 1)(send_tile)
    for i in range(remote_peers):
        send_last(i).start()

    mine = jnp.concatenate(lower + [most, mass, jnp.zeros((LANES - n - 2, pair), F32)], axis=0)
    cols[...] = mine.T
    mine = cols[pl.ds(pl.multiple_of(c * own, own), own), :]
    top[...] = jnp.broadcast_to(mine[:, n:n + 1], (own, TILE))
    scale = 1.0 / jnp.broadcast_to(mine[:, n + 1:n + 2], (own, TILE))
    inv_s[...] = scale
    for i in range(n):
        d = source(i) if i < n - 1 else me
        start = jnp.sum(jnp.where(lane == d, mine, 0.0), axis=1, keepdims=True)
        carry[i] = jnp.broadcast_to(start, (own, TILE)) * scale

    def finish(i, d, t, count, read):
        e = jnp.concatenate([jnp.exp(read(t + k) - top[...]) * inv_s[...] for k in range(count)], axis=0)
        run = running_sum(e, tri[...])
        base = carry[i]
        for k in range(count):
            part = run[k * own:(k + 1) * own, :]
            col = pl.multiple_of(d * vocab + (t + k) * TILE, TILE)
            table[:, pl.ds(col, TILE)] = part + base
            base = base + jnp.broadcast_to(part[:, TILE - 1:], (own, TILE))
        carry[i] = base

    my_rows = pl.ds(pl.multiple_of(held(0) + c * own, own), own)

    @pl.loop(0, tiles // GROUP)
    def _(g):
        finish(n - 1, me, g * GROUP, GROUP, lambda t: z[t, my_rows, :])

    def source_at(i):
        d = jnp.int32(0)
        for k in range(n - 1):
            d = d + jnp.where(i == k, source(k), 0)
        return d

    def step(i, t, count):
        finish(i, source_at(i), t, count, lambda u: land[i, u])

    counted(land.at[remote_peers], near_sem)

    @pl.loop(0, tiles // GROUP)
    def _(k):
        step(remote_peers, k * GROUP, GROUP)

    for k in range(len(WAITS) - 1):
        first, size = firsts[k], WAITS[k]
        count = min(size, GROUP)
        counted(land.at[pl.ds(0, remote_peers), pl.ds(first, size)], recv_sem.at[k])

        @pl.loop(0, remote_peers * (size // count))
        def _(u):
            step(lax.rem(u, remote_peers), first + (u // remote_peers) * count, count)

    counted(pick.at[pl.ds(0, chips - 1)], pick_recv)
    for j in range(chips):
        picked[:, j * pair:(j + 1) * pair] = pick[j]
    counted(last, recv_sem.at[len(WAITS) - 1])
    counted(land, send_sem)
    counted(stats.at[pl.ds(0, n - 1)], stat_send)
    counted(pick.at[pl.ds(0, chips - 1)], pick_send)


def write_out(chips, table, picked, last, top, inv_s, carry, table_hbm, picked_hbm, done, sem):
    n = 2 * chips
    me = lax.axis_index("vp")
    x, c = me // 2, me % 2
    own, width = table.shape
    vocab = width // n
    bulk = vocab - TILE

    def put(d, first, size, sem, source=None):
        cs = pl.ds(pl.multiple_of(d * vocab + first, TILE), size)
        return pltpu.make_async_copy(table.at[:, cs] if source is None else source, table_hbm.at[:, cs], sem)

    step = bulk // 3
    for d in range(n):
        for k in range(3):
            put(d, k * step, step, sem.at[0]).start()
    for d in (me, source_of(chips, x, c, n - 2)):
        put(d, bulk, TILE, sem.at[1]).start()
    picked_copy = pltpu.make_async_copy(picked, picked_hbm, sem.at[2])
    picked_copy.start()
    e = jnp.concatenate([jnp.exp(last[i] - top[...]) * inv_s[...] for i in range(n - 2)], axis=0)
    run = running_sum(e, triangle())
    for i in range(n - 2):
        done[i] = run[i * own:(i + 1) * own, :] + carry[i]
    for i in range(n - 2):
        put(source_of(chips, x, c, i), bulk, TILE, sem.at[1], done.at[i]).start()
    picked_copy.wait()
    put(0, 0, n * bulk, sem.at[0]).wait()
    put(0, 0, n * TILE, sem.at[1]).wait()


def solution(mesh):
    n = mesh.shape["vp"]
    chips = n // 2

    def local_step(hidden, w_local, inv_temp, target_ids):
        batch, depth = hidden.shape
        vocab = w_local.shape[1]
        tiles = vocab // TILE
        own = batch // n
        hbm = pl.BlockSpec(memory_space=pltpu.HBM)
        vmem = pl.BlockSpec(memory_space=pltpu.VMEM)
        dma = pltpu.SemaphoreType.DMA
        out = (pltpu.VMEM((own, n * vocab), F32), pltpu.VMEM((1, batch), F32), pltpu.VMEM((n - 2, own, TILE), F32),
               pltpu.VMEM((own, TILE), F32), pltpu.VMEM((own, TILE), F32), pltpu.VMEM((n, own, TILE), F32))
        parts = pl.pallas_call(
            functools.partial(kernel, chips),
            out_shape=out,
            in_specs=[hbm] * 4,
            out_specs=(vmem,) * len(out),
            scratch_shapes=[
                pltpu.VMEM((batch, depth), BF16),
                pltpu.VMEM((2, depth, TILE), BF16),
                pltpu.VMEM((tiles, batch, TILE), F32),
                pltpu.VMEM((n - 1, tiles, own, TILE), F32),
                pltpu.VMEM((1, batch), F32),
                pltpu.VMEM((1, batch), jnp.int32),
                pltpu.VMEM((batch, LANES), F32),
                pltpu.VMEM((batch, LANES), jnp.int32),
                pltpu.VMEM((batch, LANES), F32),
                pltpu.VMEM((chips, 4, 2 * own), F32),
                pltpu.VMEM((n, 4, 2 * own), F32),
                pltpu.VMEM((chips, 1, 2 * own), F32),
                pltpu.VMEM((2 * own, LANES), F32),
                pltpu.VMEM((TILE, TILE), BF16),
                dma((chips + 1,)), dma((2,)), dma((2,)), dma, dma((len(WAITS),)), dma,
                dma, dma, dma, dma,
            ],
            compiler_params=pltpu.CompilerParams(
                collective_id=0, has_side_effects=True, vmem_limit_bytes=52 * 2**20),
        )(hidden, w_local, inv_temp.reshape(1, batch), target_ids.reshape(1, batch))
        table, picked = pl.pallas_call(
            functools.partial(write_out, chips),
            out_shape=(pltpu.HBM((own, n * vocab), F32), pltpu.HBM((1, batch), F32)),
            in_specs=[vmem] * len(out),
            out_specs=(hbm, hbm),
            scratch_shapes=[pltpu.VMEM((n - 2, own, TILE), F32), dma((3,))],
            compiler_params=pltpu.CompilerParams(vmem_limit_bytes=8 * 2**20),
        )(*parts)
        return table, picked.reshape(batch)

    return jax.shard_map(
        local_step,
        mesh=mesh,
        in_specs=(P("dp", None), P(None, "vp"), P("dp"), P("dp")),
        out_specs=(P(("dp", "vp"), None), P("dp")),
        check_vma=False,
    )
```

```python
import functools

import jax
import jax.numpy as jnp
from jax import lax
from jax.experimental import pallas as pl
from jax.experimental.pallas import tpu as pltpu
from jax.sharding import PartitionSpec as P

MESH = pl.DeviceIdType.MESH
F32 = jnp.float32
BF16 = jnp.bfloat16
TILE = 256
LANES = 128
GROUP = 4
WAITS = (8, 4, 3, 1)
PEERS = ((2, 0), (2, 1), (1, 0), (3, 0), (1, 1), (3, 1), (0, 1))
CHIP_ORDER = (2, 1, 3, 0)


def peer_of(chips, x, c, i):
    dx, dc = PEERS[i]
    return lax.rem(x + dx, chips) * 2 + lax.rem(c + dc, 2)


def source_of(chips, x, c, i):
    dx, dc = PEERS[i]
    return lax.rem(x + chips - dx, chips) * 2 + lax.rem(c + dc, 2)


def triangle():
    row_id = lax.broadcasted_iota(jnp.int32, (TILE, TILE), 0)
    col_id = lax.broadcasted_iota(jnp.int32, (TILE, TILE), 1)
    return jnp.where(row_id <= col_id, 1.0, 0.0).astype(BF16)


def running_sum(e, tri):
    hi = e.astype(BF16)
    rest = e - hi.astype(F32)
    mid = rest.astype(BF16)
    low = (rest - mid.astype(F32)).astype(BF16)
    run = jnp.dot(hi, tri, preferred_element_type=F32)
    run = run + jnp.dot(mid, tri, preferred_element_type=F32)
    return run + jnp.dot(low, tri, preferred_element_type=F32)


def kernel(chips, h_hbm, w_hbm, temp_hbm, ids_hbm, table, picked, last, top, inv_s, carry,
           h, w, z, land, temp_row, ids_row, temp, ids, peak, stat_out, stats, pick, cols, tri,
           h_sem, w_sem, row_sem, send_sem, recv_sem, near_sem, stat_send, stat_recv, pick_send, pick_recv):
    n = 2 * chips
    me = lax.axis_index("vp")
    x, c = me // 2, me % 2
    batch, depth = h_hbm.shape
    vocab = w_hbm.shape[1]
    tiles = vocab // TILE
    own = batch // n
    pair = 2 * own
    remote_peers = n - 2
    firsts = [sum(WAITS[:k]) for k in range(len(WAITS))]

    def peer(i):
        return peer_of(chips, x, c, i)

    def source(i):
        return source_of(chips, x, c, i)

    def held(dx):
        return CHIP_ORDER.index(dx) * pair

    def peer_rows(i):
        dx, dc = PEERS[i]
        return pl.ds(pl.multiple_of(held(dx) + lax.rem(c + dc, 2) * own, own), own)

    def whole_rows(j):
        return pl.ds(pl.multiple_of(lax.rem(x + CHIP_ORDER[j], chips) * pair, pair), pair)

    def h_copy(j):
        return pltpu.make_async_copy(h_hbm.at[whole_rows(j), :], h.at[j * pair:(j + 1) * pair, :], h_sem.at[j])

    def turned(row):
        parts = [row[:, whole_rows(j)] for j in range(chips)]
        return jnp.broadcast_to(jnp.concatenate(parts, axis=1), (LANES, batch)).T

    def w_copy(t):
        col = pl.multiple_of(lax.rem(t, tiles) * TILE, TILE)
        slot = lax.rem(t, 2)
        return pltpu.make_async_copy(w_hbm.at[:, pl.ds(col, TILE)], w.at[slot], w_sem.at[slot])

    first_w = pltpu.make_async_copy(w_hbm.at[:, :LANES], w.at[0, :, :LANES], w_sem.at[1])
    def far_copy(core):
        r = pl.multiple_of((lax.rem(x + 2, chips) * 2 + core) * own, own)
        sem = h_sem.at[chips] if core else h_sem.at[0]
        return pltpu.make_async_copy(h_hbm.at[pl.ds(r, own), :], h.at[core * own:(core + 1) * own, :], sem)

    second_w = pltpu.make_async_copy(w_hbm.at[:, LANES:TILE], w.at[0, :, LANES:], w_sem.at[0])

    def remote(src, dst, send, recv, to):
        return pltpu.make_async_remote_copy(
            src_ref=src, dst_ref=dst, send_sem=send, recv_sem=recv, device_id={"vp": to}, device_id_type=MESH)

    def counter(t):
        k = 0
        for first in firsts[1:]:
            k = k + jnp.where(t >= first, 1, 0)
        return k

    def arrival(i, t):
        return near_sem if i == remote_peers else recv_sem.at[counter(t)]

    def send(i, t):
        return remote(z.at[t, peer_rows(i), :], land.at[i, t], send_sem, arrival(i, t), peer(i))

    def send_last(i):
        return remote(z.at[tiles - 1, peer_rows(i), :], last.at[i], send_sem, arrival(i, tiles - 1), peer(i))

    def send_last_to(dx, core):
        slot = PEERS.index((dx, 0)) + (1 if dx == 2 else 2) * lax.rem(core + c, 2)
        r = CHIP_ORDER.index(dx) * pair + core * own
        remote(z.at[tiles - 1, r:r + own, :], last.at[slot], send_sem, recv_sem.at[len(WAITS) - 1],
               lax.rem(x + dx, chips) * 2 + core).start()

    def send_tile(t):
        for i in range(remote_peers):
            send(i, t).start()

    def send_stat(i):
        at = stat_out.at[CHIP_ORDER.index(PEERS[i][0])]
        return remote(at, stats.at[me], stat_send, stat_recv, peer(i))

    def send_pick(dx):
        to = lax.rem(x + dx, chips) * 2 + c
        return remote(pick.at[x], pick.at[x], pick_send, pick_recv, to)

    def counted(ref, sem):
        pltpu.make_async_copy(ref, ref, sem).wait()

    temp_copy = pltpu.make_async_copy(temp_hbm, temp_row, row_sem.at[0])
    ids_copy = pltpu.make_async_copy(ids_hbm, ids_row, row_sem.at[1])
    first_w.start()
    for core in range(2):
        far_copy(core).start()
    temp_copy.start()
    barrier = pltpu.get_barrier_semaphore()
    for i in range(n - 1):
        pl.semaphore_signal(barrier, inc=1, device_id={"vp": peer(i)}, device_id_type=MESH)
    second_w.start()
    for j in (1, 2):
        h_copy(j).start()
    temp_copy.wait()
    temp[...] = turned(temp_row)

    first_w.wait()
    far_copy(0).wait()
    def far_part(core, half):
        rs, ls = slice(core * own, (core + 1) * own), slice(half * LANES, (half + 1) * LANES)
        acc = jnp.dot(h[rs, :], w[0, :, ls], preferred_element_type=F32) * temp[rs, :]
        z[0, rs, ls] = acc
        peak[rs, :] = jnp.maximum(peak[rs, :], acc) if half else acc

    def far_send(core, half):
        ls = slice(half * LANES, (half + 1) * LANES)
        slot = lax.rem(core + c, 2)
        remote(z.at[0, core * own:(core + 1) * own, ls], land.at[slot, 0, :, ls], send_sem, recv_sem.at[0],
               lax.rem(x + 2, chips) * 2 + core).start()

    far_part(0, 0)
    pl.semaphore_wait(barrier, n - 1)
    far_send(0, 0)
    far_copy(1).wait()
    far_part(1, 0)
    far_send(1, 0)
    w_copy(1).start()
    h_copy(3).start()
    ids_copy.start()
    second_w.wait()
    for core in range(2):
        far_part(core, 1)
        far_send(core, 1)

    def tile_rows(t, slot, rs):
        acc = jnp.dot(h[rs, :], w[slot], preferred_element_type=F32)
        by = temp[rs, :]
        left, right = acc[:, :LANES] * by, acc[:, LANES:] * by
        z[t, rs, :LANES] = left
        z[t, rs, LANES:] = right
        return jnp.maximum(left, right)

    h_copy(1).wait()
    h_copy(2).wait()
    near = pl.ds(pair, 2 * pair)
    peak[near, :] = tile_rows(0, 0, near)
    for i in range(2, remote_peers):
        send(i, 0).start()
    here = pl.ds(3 * pair, pair)
    peak[here, :] = jnp.full((pair, LANES), -jnp.inf, F32)
    h_copy(3).wait()

    @pl.loop(1, tiles)
    def _(t):
        w_copy(t + 1).start()
        w_copy(t).wait()
        best = tile_rows(t, lax.rem(t, 2), pl.ds(0, batch))
        send(remote_peers, t).start()

        @pl.when(lax.rem(t, 2) == 1)
        def _():
            send_tile((t + 1) // 2)
        peak[...] = jnp.maximum(peak[...], best)

    w_copy(tiles).wait()
    peak[here, :] = jnp.maximum(peak[here, :], tile_rows(0, 0, here))
    send(remote_peers, 0).start()

    ids_copy.wait()
    ids[...] = turned(ids_row)
    lane = lax.broadcasted_iota(jnp.int32, (own, LANES), 1)

    @pl.loop(0, n)
    def _(b):
        rs = pl.ds(pl.multiple_of(b * own, own), own)
        most = jnp.broadcast_to(jnp.max(peak[rs, :], axis=1, keepdims=True), (own, LANES))
        target = ids[rs, :] - (me * vocab) - lane

        def add(t, sums):
            total, below = sums
            for half in range(2):
                e = jnp.exp(z[t, rs, half * LANES:(half + 1) * LANES] - most)
                total = total + e
                below = below + jnp.where(target >= t * TILE + half * LANES, e, 0.0)
            return total, below

        zero = jnp.zeros((own, LANES), F32)
        total, below = lax.fori_loop(0, tiles, add, (zero, zero))
        total = jnp.sum(total, axis=1, keepdims=True)
        below = jnp.sum(below, axis=1, keepdims=True)
        peak[rs, :] = jnp.where(lane == 0, most, jnp.where(lane == 1, total, below))

    flipped = peak[...].T
    for j in range(chips):
        stat_out[j] = flipped[:4, j * pair:(j + 1) * pair]
    stats[me] = stat_out[CHIP_ORDER.index(0)]
    for i in range(n - 1):
        send_stat(i).start()

    sent = tiles // 2 + 1
    pl.loop(sent, sent + 3)(send_tile)
    tri[...] = triangle()
    counted(stats.at[pl.ds(0, n - 1)], stat_recv)

    most = stats[0, 0:1, :]
    for d in range(1, n):
        most = jnp.maximum(most, stats[d, 0:1, :])
    mass = jnp.zeros_like(most)
    below = jnp.zeros_like(most)
    lower = []
    for d in range(n):
        lower.append(mass)
        scale = jnp.exp(stats[d, 0:1, :] - most)
        mass = mass + stats[d, 1:2, :] * scale
        below = below + stats[d, 2:3, :] * scale
    pick[x] = below / mass
    for dx in range(1, chips):
        send_pick(dx).start()
    pl.loop(sent + 3, tiles - 1)(send_tile)
    send_last(0).start()
    send_last(1).start()
    send_last_to(1, 1)
    send_last(3).start()
    send_last_to(1, 0)
    send_last(5).start()

    mine = jnp.concatenate(lower + [most, mass, jnp.zeros((LANES - n - 2, pair), F32)], axis=0)
    cols[...] = mine.T
    mine = cols[pl.ds(pl.multiple_of(c * own, own), own), :]
    top[...] = jnp.broadcast_to(mine[:, n:n + 1], (own, TILE))
    scale = 1.0 / jnp.broadcast_to(mine[:, n + 1:n + 2], (own, TILE))
    inv_s[...] = scale
    for i in range(n):
        d = source(i) if i < n - 1 else me
        start = jnp.sum(jnp.where(lane == d, mine, 0.0), axis=1, keepdims=True)
        carry[i] = jnp.broadcast_to(start, (own, TILE)) * scale

    def finish(i, d, t, count, read):
        e = jnp.concatenate([jnp.exp(read(t + k) - top[...]) * inv_s[...] for k in range(count)], axis=0)
        run = running_sum(e, tri[...])
        base = carry[i]
        for k in range(count):
            part = run[k * own:(k + 1) * own, :]
            col = pl.multiple_of(d * vocab + (t + k) * TILE, TILE)
            table[:, pl.ds(col, TILE)] = part + base
            base = base + jnp.broadcast_to(part[:, TILE - 1:], (own, TILE))
        carry[i] = base

    my_rows = pl.ds(pl.multiple_of(held(0) + c * own, own), own)

    @pl.loop(0, tiles // GROUP)
    def _(g):
        finish(n - 1, me, g * GROUP, GROUP, lambda t: z[t, my_rows, :])

    def source_at(i):
        d = jnp.int32(0)
        for k in range(n - 1):
            d = d + jnp.where(i == k, source(k), 0)
        return d

    def step(i, t, count):
        finish(i, source_at(i), t, count, lambda u: land[i, u])

    counted(land.at[remote_peers], near_sem)

    @pl.loop(0, tiles // GROUP)
    def _(k):
        step(remote_peers, k * GROUP, GROUP)

    for k in range(len(WAITS) - 1):
        first, size = firsts[k], WAITS[k]
        count = min(size, GROUP)
        counted(land.at[pl.ds(0, remote_peers), pl.ds(first, size)], recv_sem.at[k])

        @pl.loop(0, remote_peers * (size // count))
        def _(u):
            step(lax.rem(u, remote_peers), first + (u // remote_peers) * count, count)

    counted(pick.at[pl.ds(0, chips - 1)], pick_recv)
    for j in range(chips):
        picked[:, j * pair:(j + 1) * pair] = pick[j]
    counted(last, recv_sem.at[len(WAITS) - 1])
    counted(land, send_sem)
    counted(stats.at[pl.ds(0, n - 1)], stat_send)
    counted(pick.at[pl.ds(0, chips - 1)], pick_send)


def write_out(chips, table, picked, last, top, inv_s, carry, table_hbm, picked_hbm, done, sem):
    n = 2 * chips
    me = lax.axis_index("vp")
    x, c = me // 2, me % 2
    own, width = table.shape
    vocab = width // n
    bulk = vocab - TILE

    def put(d, first, size, sem, source=None):
        cs = pl.ds(pl.multiple_of(d * vocab + first, TILE), size)
        return pltpu.make_async_copy(table.at[:, cs] if source is None else source, table_hbm.at[:, cs], sem)

    step = bulk // 3
    for d in range(n):
        for k in range(3):
            put(d, k * step, step, sem.at[0]).start()
    for d in (me, source_of(chips, x, c, n - 2)):
        put(d, bulk, TILE, sem.at[1]).start()
    picked_copy = pltpu.make_async_copy(picked, picked_hbm, sem.at[2])
    picked_copy.start()
    e = jnp.concatenate([jnp.exp(last[i] - top[...]) * inv_s[...] for i in range(n - 2)], axis=0)
    run = running_sum(e, triangle())
    for i in range(n - 2):
        done[i] = run[i * own:(i + 1) * own, :] + carry[i]
    for i in range(n - 2):
        put(source_of(chips, x, c, i), bulk, TILE, sem.at[1], done.at[i]).start()
    picked_copy.wait()
    put(0, 0, n * bulk, sem.at[0]).wait()
    put(0, 0, n * TILE, sem.at[1]).wait()


def solution(mesh):
    n = mesh.shape["vp"]
    chips = n // 2

    def local_step(hidden, w_local, inv_temp, target_ids):
        batch, depth = hidden.shape
        vocab = w_local.shape[1]
        tiles = vocab // TILE
        own = batch // n
        hbm = pl.BlockSpec(memory_space=pltpu.HBM)
        vmem = pl.BlockSpec(memory_space=pltpu.VMEM)
        dma = pltpu.SemaphoreType.DMA
        out = (pltpu.VMEM((own, n * vocab), F32), pltpu.VMEM((1, batch), F32), pltpu.VMEM((n - 2, own, TILE), F32),
               pltpu.VMEM((own, TILE), F32), pltpu.VMEM((own, TILE), F32), pltpu.VMEM((n, own, TILE), F32))
        parts = pl.pallas_call(
            functools.partial(kernel, chips),
            out_shape=out,
            in_specs=[hbm] * 4,
            out_specs=(vmem,) * len(out),
            scratch_shapes=[
                pltpu.VMEM((batch, depth), BF16),
                pltpu.VMEM((2, depth, TILE), BF16),
                pltpu.VMEM((tiles, batch, TILE), F32),
                pltpu.VMEM((n - 1, tiles, own, TILE), F32),
                pltpu.VMEM((1, batch), F32),
                pltpu.VMEM((1, batch), jnp.int32),
                pltpu.VMEM((batch, LANES), F32),
                pltpu.VMEM((batch, LANES), jnp.int32),
                pltpu.VMEM((batch, LANES), F32),
                pltpu.VMEM((chips, 4, 2 * own), F32),
                pltpu.VMEM((n, 4, 2 * own), F32),
                pltpu.VMEM((chips, 1, 2 * own), F32),
                pltpu.VMEM((2 * own, LANES), F32),
                pltpu.VMEM((TILE, TILE), BF16),
                dma((chips + 1,)), dma((2,)), dma((2,)), dma, dma((len(WAITS),)), dma,
                dma, dma, dma, dma,
            ],
            compiler_params=pltpu.CompilerParams(
                collective_id=0, has_side_effects=True, vmem_limit_bytes=52 * 2**20),
        )(hidden, w_local, inv_temp.reshape(1, batch), target_ids.reshape(1, batch))
        table, picked = pl.pallas_call(
            functools.partial(write_out, chips),
            out_shape=(pltpu.HBM((own, n * vocab), F32), pltpu.HBM((1, batch), F32)),
            in_specs=[vmem] * len(out),
            out_specs=(hbm, hbm),
            scratch_shapes=[pltpu.VMEM((n - 2, own, TILE), F32), dma((3,))],
            compiler_params=pltpu.CompilerParams(vmem_limit_bytes=8 * 2**20),
        )(*parts)
        return table, picked.reshape(batch)

    return jax.shard_map(
        local_step,
        mesh=mesh,
        in_specs=(P("dp", None), P(None, "vp"), P("dp"), P("dp")),
        out_specs=(P(("dp", "vp"), None), P("dp")),
        check_vma=False,
    )
```

```python
import functools

import jax
import jax.numpy as jnp
from jax import lax
from jax.experimental import pallas as pl
from jax.experimental.pallas import tpu as pltpu
from jax.sharding import PartitionSpec as P

MESH = pl.DeviceIdType.MESH
F32 = jnp.float32
BF16 = jnp.bfloat16
TILE = 256
LANES = 128
GROUP = 4
WAITS = (8, 4, 3, 1)
PEERS = ((2, 0), (2, 1), (1, 0), (3, 0), (1, 1), (3, 1), (0, 1))
CHIP_ORDER = (2, 1, 3, 0)


def peer_of(chips, x, c, i):
    dx, dc = PEERS[i]
    return lax.rem(x + dx, chips) * 2 + lax.rem(c + dc, 2)


def source_of(chips, x, c, i):
    dx, dc = PEERS[i]
    return lax.rem(x + chips - dx, chips) * 2 + lax.rem(c + dc, 2)


def triangle():
    row_id = lax.broadcasted_iota(jnp.int32, (TILE, TILE), 0)
    col_id = lax.broadcasted_iota(jnp.int32, (TILE, TILE), 1)
    return jnp.where(row_id <= col_id, 1.0, 0.0).astype(BF16)


def running_sum(e, tri):
    hi = e.astype(BF16)
    rest = e - hi.astype(F32)
    mid = rest.astype(BF16)
    low = (rest - mid.astype(F32)).astype(BF16)
    run = jnp.dot(hi, tri, preferred_element_type=F32)
    run = run + jnp.dot(mid, tri, preferred_element_type=F32)
    return run + jnp.dot(low, tri, preferred_element_type=F32)


def kernel(chips, h_hbm, w_hbm, temp_hbm, ids_hbm, table, picked, last, top, inv_s, carry,
           h, w, z, land, temp_row, ids_row, temp, ids, peak, stat_out, stats, pick, cols, tri,
           h_sem, w_sem, row_sem, send_sem, recv_sem, near_sem, stat_send, stat_recv, pick_send, pick_recv):
    n = 2 * chips
    me = lax.axis_index("vp")
    x, c = me // 2, me % 2
    batch, depth = h_hbm.shape
    vocab = w_hbm.shape[1]
    tiles = vocab // TILE
    own = batch // n
    pair = 2 * own
    remote_peers = n - 2
    firsts = [sum(WAITS[:k]) for k in range(len(WAITS))]

    def peer(i):
        return peer_of(chips, x, c, i)

    def source(i):
        return source_of(chips, x, c, i)

    def held(dx):
        return CHIP_ORDER.index(dx) * pair

    def peer_rows(i):
        dx, dc = PEERS[i]
        return pl.ds(pl.multiple_of(held(dx) + lax.rem(c + dc, 2) * own, own), own)

    def whole_rows(j):
        return pl.ds(pl.multiple_of(lax.rem(x + CHIP_ORDER[j], chips) * pair, pair), pair)

    def h_copy(j):
        return pltpu.make_async_copy(h_hbm.at[whole_rows(j), :], h.at[j * pair:(j + 1) * pair, :], h_sem.at[3 if j == 3 else 1])

    def turned(row):
        parts = [row[:, whole_rows(j)] for j in range(chips)]
        return jnp.broadcast_to(jnp.concatenate(parts, axis=1), (LANES, batch)).T

    def w_copy(t):
        col = pl.multiple_of(lax.rem(t, tiles) * TILE, TILE)
        slot = lax.rem(t, 2)
        return pltpu.make_async_copy(w_hbm.at[:, pl.ds(col, TILE)], w.at[slot], w_sem.at[slot])

    first_w = pltpu.make_async_copy(w_hbm.at[:, :LANES], w.at[0, :, :LANES], w_sem.at[1])
    def far_copy(core):
        r = pl.multiple_of((lax.rem(x + 2, chips) * 2 + core) * own, own)
        sem = h_sem.at[2] if core else h_sem.at[0]
        return pltpu.make_async_copy(h_hbm.at[pl.ds(r, own), :], h.at[core * own:(core + 1) * own, :], sem)

    second_w = pltpu.make_async_copy(w_hbm.at[:, LANES:TILE], w.at[0, :, LANES:], w_sem.at[0])

    def remote(src, dst, send, recv, to):
        return pltpu.make_async_remote_copy(
            src_ref=src, dst_ref=dst, send_sem=send, recv_sem=recv, device_id={"vp": to}, device_id_type=MESH)

    def counter(t):
        k = 0
        for first in firsts[1:]:
            k = k + jnp.where(t >= first, 1, 0)
        return k

    def arrival(i, t):
        return near_sem if i == remote_peers else recv_sem.at[counter(t)]

    def send(i, t):
        return remote(z.at[t, peer_rows(i), :], land.at[i, t], send_sem, arrival(i, t), peer(i))

    def send_last(i):
        return remote(z.at[tiles - 1, peer_rows(i), :], last.at[i], send_sem, arrival(i, tiles - 1), peer(i))

    def send_last_to(dx, core):
        slot = PEERS.index((dx, 0)) + (1 if dx == 2 else 2) * lax.rem(core + c, 2)
        r = CHIP_ORDER.index(dx) * pair + core * own
        remote(z.at[tiles - 1, r:r + own, :], last.at[slot], send_sem, recv_sem.at[len(WAITS) - 1],
               lax.rem(x + dx, chips) * 2 + core).start()

    def send_tile(t):
        for i in range(remote_peers):
            send(i, t).start()

    def send_stat(i):
        at = stat_out.at[CHIP_ORDER.index(PEERS[i][0])]
        return remote(at, stats.at[me], stat_send, stat_recv, peer(i))

    def send_pick(dx):
        to = lax.rem(x + dx, chips) * 2 + c
        return remote(pick.at[x], pick.at[x], pick_send, pick_recv, to)

    def counted(ref, sem):
        pltpu.make_async_copy(ref, ref, sem).wait()

    temp_copy = pltpu.make_async_copy(temp_hbm, temp_row, row_sem.at[0])
    ids_copy = pltpu.make_async_copy(ids_hbm, ids_row, row_sem.at[1])
    first_w.start()
    for core in range(2):
        far_copy(core).start()
    temp_copy.start()
    barrier = pltpu.get_barrier_semaphore()
    for i in range(n - 1):
        pl.semaphore_signal(barrier, inc=1, device_id={"vp": peer(i)}, device_id_type=MESH)
    second_w.start()
    for j in (1, 2):
        h_copy(j).start()
    temp_copy.wait()
    temp[...] = turned(temp_row)

    first_w.wait()
    far_copy(0).wait()
    def far_part(core, half):
        rs, ls = slice(core * own, (core + 1) * own), slice(half * LANES, (half + 1) * LANES)
        acc = jnp.dot(h[rs, :], w[0, :, ls], preferred_element_type=F32) * temp[rs, :]
        z[0, rs, ls] = acc
        peak[rs, :] = jnp.maximum(peak[rs, :], acc) if half else acc

    def far_send(core, half):
        ls = slice(half * LANES, (half + 1) * LANES)
        slot = lax.rem(core + c, 2)
        remote(z.at[0, core * own:(core + 1) * own, ls], land.at[slot, 0, :, ls], send_sem, recv_sem.at[0],
               lax.rem(x + 2, chips) * 2 + core).start()

    far_part(0, 0)
    pl.semaphore_wait(barrier, n - 1)
    far_send(0, 0)
    far_copy(1).wait()
    far_part(1, 0)
    far_send(1, 0)
    w_copy(1).start()
    h_copy(3).start()
    ids_copy.start()
    second_w.wait()
    for core in range(2):
        far_part(core, 1)
        far_send(core, 1)

    def tile_rows(t, slot, rs):
        acc = jnp.dot(h[rs, :], w[slot], preferred_element_type=F32)
        by = temp[rs, :]
        left, right = acc[:, :LANES] * by, acc[:, LANES:] * by
        z[t, rs, :LANES] = left
        z[t, rs, LANES:] = right
        return jnp.maximum(left, right)

    counted(h.at[pair:3 * pair, :], h_sem.at[1])
    near = pl.ds(pair, 2 * pair)
    peak[near, :] = tile_rows(0, 0, near)
    for i in range(2, remote_peers):
        send(i, 0).start()
    here = pl.ds(3 * pair, pair)
    peak[here, :] = jnp.full((pair, LANES), -jnp.inf, F32)
    h_copy(3).wait()

    @pl.loop(1, tiles)
    def _(t):
        w_copy(t + 1).start()
        w_copy(t).wait()
        best = tile_rows(t, lax.rem(t, 2), pl.ds(0, batch))
        send(remote_peers, t).start()

        @pl.when(lax.rem(t, 2) == 1)
        def _():
            send_tile((t + 1) // 2)
        peak[...] = jnp.maximum(peak[...], best)

    w_copy(tiles).wait()
    peak[here, :] = jnp.maximum(peak[here, :], tile_rows(0, 0, here))
    send(remote_peers, 0).start()

    ids_copy.wait()
    ids[...] = turned(ids_row)
    lane = lax.broadcasted_iota(jnp.int32, (own, LANES), 1)

    @pl.loop(0, n)
    def _(b):
        rs = pl.ds(pl.multiple_of(b * own, own), own)
        most = jnp.broadcast_to(jnp.max(peak[rs, :], axis=1, keepdims=True), (own, LANES))
        target = ids[rs, :] - (me * vocab) - lane

        def add(t, sums):
            total, below = sums
            for half in range(2):
                e = jnp.exp(z[t, rs, half * LANES:(half + 1) * LANES] - most)
                total = total + e
                below = below + jnp.where(target >= t * TILE + half * LANES, e, 0.0)
            return total, below

        zero = jnp.zeros((own, LANES), F32)
        total, below = lax.fori_loop(0, tiles, add, (zero, zero))
        total = jnp.sum(total, axis=1, keepdims=True)
        below = jnp.sum(below, axis=1, keepdims=True)
        peak[rs, :] = jnp.where(lane == 0, most, jnp.where(lane == 1, total, below))

    flipped = peak[...].T
    for j in range(chips):
        stat_out[j] = flipped[:4, j * pair:(j + 1) * pair]
    stats[me] = stat_out[CHIP_ORDER.index(0)]
    for i in range(n - 1):
        send_stat(i).start()

    sent = tiles // 2 + 1
    pl.loop(sent, sent + 3)(send_tile)
    tri[...] = triangle()
    counted(stats.at[pl.ds(0, n - 1)], stat_recv)

    most = stats[0, 0:1, :]
    for d in range(1, n):
        most = jnp.maximum(most, stats[d, 0:1, :])
    mass = jnp.zeros_like(most)
    below = jnp.zeros_like(most)
    lower = []
    for d in range(n):
        lower.append(mass)
        scale = jnp.exp(stats[d, 0:1, :] - most)
        mass = mass + stats[d, 1:2, :] * scale
        below = below + stats[d, 2:3, :] * scale
    pick[x] = below / mass
    for dx in range(1, chips):
        send_pick(dx).start()
    pl.loop(sent + 3, tiles - 1)(send_tile)
    send_last(0).start()
    send_last(1).start()
    send_last_to(1, 1)
    send_last(3).start()
    send_last_to(1, 0)
    send_last(5).start()

    mine = jnp.concatenate(lower + [most, mass, jnp.zeros((LANES - n - 2, pair), F32)], axis=0)
    cols[...] = mine.T
    mine = cols[pl.ds(pl.multiple_of(c * own, own), own), :]
    top[...] = jnp.broadcast_to(mine[:, n:n + 1], (own, TILE))
    scale = 1.0 / jnp.broadcast_to(mine[:, n + 1:n + 2], (own, TILE))
    inv_s[...] = scale
    for i in range(n):
        d = source(i) if i < n - 1 else me
        start = jnp.sum(jnp.where(lane == d, mine, 0.0), axis=1, keepdims=True)
        carry[i] = jnp.broadcast_to(start, (own, TILE)) * scale

    def finish(i, d, t, count, read):
        e = jnp.concatenate([jnp.exp(read(t + k) - top[...]) * inv_s[...] for k in range(count)], axis=0)
        run = running_sum(e, tri[...])
        base = carry[i]
        for k in range(count):
            part = run[k * own:(k + 1) * own, :]
            col = pl.multiple_of(d * vocab + (t + k) * TILE, TILE)
            table[:, pl.ds(col, TILE)] = part + base
            base = base + jnp.broadcast_to(part[:, TILE - 1:], (own, TILE))
        carry[i] = base

    my_rows = pl.ds(pl.multiple_of(held(0) + c * own, own), own)

    @pl.loop(0, tiles // GROUP)
    def _(g):
        finish(n - 1, me, g * GROUP, GROUP, lambda t: z[t, my_rows, :])

    def source_at(i):
        d = jnp.int32(0)
        for k in range(n - 1):
            d = d + jnp.where(i == k, source(k), 0)
        return d

    def step(i, t, count):
        finish(i, source_at(i), t, count, lambda u: land[i, u])

    counted(land.at[remote_peers], near_sem)

    @pl.loop(0, tiles // GROUP)
    def _(k):
        step(remote_peers, k * GROUP, GROUP)

    for k in range(len(WAITS) - 1):
        first, size = firsts[k], WAITS[k]
        count = min(size, GROUP)
        counted(land.at[pl.ds(0, remote_peers), pl.ds(first, size)], recv_sem.at[k])

        @pl.loop(0, remote_peers * (size // count))
        def _(u):
            step(lax.rem(u, remote_peers), first + (u // remote_peers) * count, count)

    counted(pick.at[pl.ds(0, chips - 1)], pick_recv)
    for j in range(chips):
        picked[:, j * pair:(j + 1) * pair] = pick[j]
    counted(last, recv_sem.at[len(WAITS) - 1])
    counted(land, send_sem)
    counted(stats.at[pl.ds(0, n - 1)], stat_send)
    counted(pick.at[pl.ds(0, chips - 1)], pick_send)


def write_out(chips, table, picked, last, top, inv_s, carry, table_hbm, picked_hbm, done, sem):
    n = 2 * chips
    me = lax.axis_index("vp")
    x, c = me // 2, me % 2
    own, width = table.shape
    vocab = width // n
    bulk = vocab - TILE

    def put(d, first, size, sem, source=None):
        cs = pl.ds(pl.multiple_of(d * vocab + first, TILE), size)
        return pltpu.make_async_copy(table.at[:, cs] if source is None else source, table_hbm.at[:, cs], sem)

    step = bulk // 3
    for d in range(n):
        for k in range(3):
            put(d, k * step, step, sem.at[0]).start()
    for d in (me, source_of(chips, x, c, n - 2)):
        put(d, bulk, TILE, sem.at[1]).start()
    picked_copy = pltpu.make_async_copy(picked, picked_hbm, sem.at[2])
    picked_copy.start()
    e = jnp.concatenate([jnp.exp(last[i] - top[...]) * inv_s[...] for i in range(n - 2)], axis=0)
    run = running_sum(e, triangle())
    for i in range(n - 2):
        done[i] = run[i * own:(i + 1) * own, :] + carry[i]
    for i in range(n - 2):
        put(source_of(chips, x, c, i), bulk, TILE, sem.at[1], done.at[i]).start()
    picked_copy.wait()
    put(0, 0, n * bulk, sem.at[0]).wait()
    put(0, 0, n * TILE, sem.at[1]).wait()


def solution(mesh):
    n = mesh.shape["vp"]
    chips = n // 2

    def local_step(hidden, w_local, inv_temp, target_ids):
        batch, depth = hidden.shape
        vocab = w_local.shape[1]
        tiles = vocab // TILE
        own = batch // n
        hbm = pl.BlockSpec(memory_space=pltpu.HBM)
        vmem = pl.BlockSpec(memory_space=pltpu.VMEM)
        dma = pltpu.SemaphoreType.DMA
        out = (pltpu.VMEM((own, n * vocab), F32), pltpu.VMEM((1, batch), F32), pltpu.VMEM((n - 2, own, TILE), F32),
               pltpu.VMEM((own, TILE), F32), pltpu.VMEM((own, TILE), F32), pltpu.VMEM((n, own, TILE), F32))
        parts = pl.pallas_call(
            functools.partial(kernel, chips),
            out_shape=out,
            in_specs=[hbm] * 4,
            out_specs=(vmem,) * len(out),
            scratch_shapes=[
                pltpu.VMEM((batch, depth), BF16),
                pltpu.VMEM((2, depth, TILE), BF16),
                pltpu.VMEM((tiles, batch, TILE), F32),
                pltpu.VMEM((n - 1, tiles, own, TILE), F32),
                pltpu.VMEM((1, batch), F32),
                pltpu.VMEM((1, batch), jnp.int32),
                pltpu.VMEM((batch, LANES), F32),
                pltpu.VMEM((batch, LANES), jnp.int32),
                pltpu.VMEM((batch, LANES), F32),
                pltpu.VMEM((chips, 4, 2 * own), F32),
                pltpu.VMEM((n, 4, 2 * own), F32),
                pltpu.VMEM((chips, 1, 2 * own), F32),
                pltpu.VMEM((2 * own, LANES), F32),
                pltpu.VMEM((TILE, TILE), BF16),
                dma((chips,)), dma((2,)), dma((2,)), dma, dma((len(WAITS),)), dma,
                dma, dma, dma, dma,
            ],
            compiler_params=pltpu.CompilerParams(
                collective_id=0, has_side_effects=True, vmem_limit_bytes=52 * 2**20),
        )(hidden, w_local, inv_temp.reshape(1, batch), target_ids.reshape(1, batch))
        table, picked = pl.pallas_call(
            functools.partial(write_out, chips),
            out_shape=(pltpu.HBM((own, n * vocab), F32), pltpu.HBM((1, batch), F32)),
            in_specs=[vmem] * len(out),
            out_specs=(hbm, hbm),
            scratch_shapes=[pltpu.VMEM((n - 2, own, TILE), F32), dma((3,))],
            compiler_params=pltpu.CompilerParams(vmem_limit_bytes=8 * 2**20),
        )(*parts)
        return table, picked.reshape(batch)

    return jax.shard_map(
        local_step,
        mesh=mesh,
        in_specs=(P("dp", None), P(None, "vp"), P("dp"), P("dp")),
        out_specs=(P(("dp", "vp"), None), P("dp")),
        check_vma=False,
    )
```
